512 devices in a mesh: range: 32 (over y_hi, z), depth: 16 (over x, y_lo, core).
Axes of the slice: x: 4, y: 8 (y_hi: 4, y_lo: 2; y = y_hi * 2 + y_lo), z: 8, core: 2. Of those that a mesh axis runs over, the one named last changes fastest.
Arguments:
- pressure: float32 [16384, 4096], P('depth', 'range'), may hold values from -6 to 6
- vel_range: float32 [16384, 4096], P('depth', 'range'), may hold values from -3 to 3
- vel_depth: float32 [16384, 4096], P('depth', 'range'), may hold values from -3 to 3
- sound_speed: float32 [16384, 4096], P('depth', 'range'), may hold values from 0.5 to 1.1
- density: float32 [16384, 4096], P('depth', 'range'), may hold values from 1 to 3
- ahead_speed: float32 [16384, 64], P('depth'), may hold values from 0.5 to 1.1
- ahead_density: float32 [16384, 64], P('depth'), may hold values from 1 to 3
- shifts: int32 [4], replicated, may hold values from 1 to 16, as said below
- sources: int32 [8, 2], replicated, may hold values from 0 to 16383, as said below
- wavelet: float32 [8, 4], replicated, may hold values from -12 to 12
Outputs:
- pressure_out: float32 [16384, 4096], P('depth', 'range')
- range_out: float32 [16384, 4096], P('depth', 'range')
- depth_out: float32 [16384, 4096], P('depth', 'range')
The draws below stay inside these ranges and needn't reach their ends.
Inputs may be any that keep to these rules, and one draw needn't show every extreme that they name: `shifts`: every draw has a step that advances by exactly 16 columns. `sources`: column 0 is a depth index below 16384, column 1 a range index below 4096.
All inputs are finite; a program needn't handle non-finite values.
Results may differ from the reference program's by a relative error of at most 0.0003.
Values sent between devices are 32-bit elements; how exact they have to be, the bound alone decides.
A program may use at most 64 MiB of HBM per device.

```python
import math
import jax
import jax.numpy as jnp
from jax import lax

SMAX = 16
ITERS = 4
NSRC = 8
NZ = 16384
NR = 4096
AHEAD = 64


def draw_shifts(key, part):
    first, second = jax.random.split(jax.random.fold_in(key, 11))
    base = jax.random.randint(first, (ITERS,), 1, SMAX + 1)
    chosen = jax.random.randint(second, (), 0, ITERS)
    return jnp.where(jnp.arange(ITERS) == chosen, SMAX, base).astype(jnp.int32)


def draw_sources(key, part):
    first, second, third = jax.random.split(jax.random.fold_in(key, 23), 3)
    depth_index = jax.random.randint(first, (NSRC,), 0, NZ)
    range_index = jax.random.randint(second, (NSRC,), 0, NR)
    order = jax.random.permutation(third, NSRC)
    slots = jnp.arange(NSRC, dtype=jnp.int32)
    depth_index = jnp.where(slots == order[0], NZ - 1, depth_index)
    depth_index = jnp.where(slots == order[2], 0, depth_index)
    range_index = jnp.where(slots == order[1], NR - 1, range_index)
    return jnp.stack([depth_index, range_index], 1).astype(jnp.int32)


def level_of(own_key, dims, cuts, smallest, top_value):
    factor_of = 1.0
    for dim, blocks in cuts:
        draws = jax.random.uniform(jax.random.fold_in(jax.random.fold_in(own_key, 6), dim), (blocks,), jnp.float32, smallest / len(cuts), top_value / len(cuts))
        factor_of = factor_of * jnp.repeat(jnp.exp(draws), dims[dim] // blocks).reshape((-1,) + (1,) * (len(dims) - 1 - dim))
    return factor_of


def bell_draw(rng, shape, width, reach, cuts=(), kind=jnp.bfloat16):
    loudness = level_of(rng, shape, cuts, -0.22, 0.18) if cuts else 1.0
    entries = jax.random.normal(rng, shape, jnp.float32) * width * loudness
    return jnp.minimum(jnp.maximum(entries, -reach), reach).astype(kind)


def setup_inputs(seed: int = 0) -> dict:
    seeds = jax.random.split(jax.random.key(seed), 11)
    return {
        "pressure": bell_draw(seeds[0], (NZ, NR), 1.0, 6.0, ((0, 16), (1, 32)), jnp.float32),
        "vel_range": bell_draw(seeds[1], (NZ, NR), 0.5, 3.0, ((0, 16), (1, 32)), jnp.float32),
        "vel_depth": bell_draw(seeds[2], (NZ, NR), 0.5, 3.0, ((0, 16), (1, 32)), jnp.float32),
        "sound_speed": jnp.clip(0.5 + 0.6 * jax.random.uniform(seeds[3], (NZ, NR), jnp.float32) ** level_of(seeds[3], (NZ, NR), ((0, 16), (1, 32)), -0.2, 0.2), 0.5, 1.1),
        "density": jnp.clip(jnp.exp(math.log(3.0) - 1.0986123 * jax.random.uniform(seeds[4], (NZ, NR), jnp.float32) ** level_of(seeds[4], (NZ, NR), ((0, 16), (1, 32)), -0.2, 0.2)), 1.0, 3.0),
        "ahead_speed": jnp.clip(0.5 + 0.6 * jax.random.uniform(seeds[5], (NZ, AHEAD), jnp.float32) ** level_of(seeds[5], (NZ, AHEAD), ((0, 16),), -0.2, 0.2), 0.5, 1.1),
        "ahead_density": jnp.clip(jnp.exp(math.log(3.0) - 1.0986123 * jax.random.uniform(seeds[6], (NZ, AHEAD), jnp.float32) ** level_of(seeds[6], (NZ, AHEAD), ((0, 16),), -0.2, 0.2)), 1.0, 3.0),
        "shifts": draw_shifts(jax.random.fold_in(seeds[10], 71), 0),
        "sources": draw_sources(jax.random.fold_in(seeds[10], 71), 0),
        "wavelet": bell_draw(seeds[9], (NSRC, ITERS), 3.0, 12.0, (), jnp.float32),
    }


TIME_STEP = 0.6


def reference(pressure, vel_range, vel_depth, sound_speed, density, ahead_speed, ahead_density, shifts, sources, wavelet):
    offset = jnp.int32(0)
    for segment in range(ITERS):
        p_right = jnp.concatenate([pressure[:, 1:], jnp.zeros_like(pressure[:, :1])], 1)
        rho_right = jnp.concatenate([density[:, 1:], density[:, -1:]], 1)
        vel_range = vel_range - TIME_STEP * (2.0 / (density + rho_right)) * (p_right - pressure)
        p_lower = jnp.concatenate([pressure[1:], jnp.zeros_like(pressure[:1])], 0)
        rho_lower = jnp.concatenate([density[1:], density[-1:]], 0)
        vel_depth = vel_depth - TIME_STEP * (2.0 / (density + rho_lower)) * (p_lower - pressure)
        range_left = jnp.concatenate([jnp.zeros_like(vel_range[:, :1]), vel_range[:, :-1]], 1)
        depth_upper = jnp.concatenate([jnp.zeros_like(vel_depth[:1]), vel_depth[:-1]], 0)
        stiffness = density * sound_speed * sound_speed
        pressure = pressure - TIME_STEP * stiffness * ((vel_range - range_left) + (vel_depth - depth_upper))
        amplitude = wavelet[:, segment]
        depth_onehot = (sources[:, 0][:, None] == jnp.arange(NZ, dtype=jnp.int32)[None, :]).astype(pressure.dtype)
        range_onehot = ((sources[:, 1] - offset)[:, None] == jnp.arange(NR, dtype=jnp.int32)[None, :]).astype(pressure.dtype)
        pressure = pressure + jnp.dot((depth_onehot * amplitude[:, None]).T, range_onehot, precision=lax.Precision.HIGHEST)
        advance_by = shifts[segment].astype(jnp.int32)
        zero_strip = jnp.zeros((NZ, SMAX), pressure.dtype)
        new_speed = lax.dynamic_slice_in_dim(ahead_speed, offset, SMAX, 1)
        new_density = lax.dynamic_slice_in_dim(ahead_density, offset, SMAX, 1)

        def advance(values, incoming):
            return lax.dynamic_slice_in_dim(jnp.concatenate([values, incoming], 1), advance_by, NR, 1)

        pressure = advance(pressure, zero_strip)
        vel_range = advance(vel_range, zero_strip)
        vel_depth = advance(vel_depth, zero_strip)
        sound_speed = advance(sound_speed, new_speed)
        density = advance(density, new_density)
        offset = offset + advance_by
    return pressure, vel_range, vel_depth
```

```python
import functools

import jax
import jax.numpy as jnp
from jax import lax
from jax.experimental import pallas as pl
from jax.experimental.pallas import tpu as pltpu
from jax.sharding import PartitionSpec as P

ITERS = 4
TIME_STEP = 0.6
MESH = pl.DeviceIdType.MESH
HALO = 8
ROWS = 128
TAIL = 64


def advance(fields, row, col, offsets, points, full, left, ends):
    p, vr, vz, c, rho = fields
    n = p.shape[0]
    a = (2.0 * TIME_STEP) / (rho + pltpu.roll(rho, 127, 1))
    b = (2.0 * TIME_STEP) / (rho + pltpu.roll(rho, n - 1, 0))
    b = jnp.where(row >= 0, b, 0.0)
    k = TIME_STEP * (rho * c * c)
    if ends:
        a_last = TIME_STEP / rho
    masks = []
    for where_row, where_col, _ in points:
        masks.append(jnp.logical_and(row == where_row, col == where_col))
    for t in range(ITERS):
        push_r = pltpu.roll(p, 127, 1) - p
        push_z = b * (pltpu.roll(p, n - 1, 0) - p)
        if ends:
            on = col < full + offsets[t]
            push_r = jnp.where(col == full + offsets[t] - 1, a_last, a) * push_r
            vr = jnp.where(on, vr - push_r, vr)
            vz = jnp.where(on, vz - push_z, vz)
        else:
            vr = vr - a * push_r
            vz = vz - push_z
        back = pltpu.roll(vr, 1, 1)
        if left:
            back = jnp.where(col == offsets[t], 0.0, back)
        fresh = p - k * ((vr - back) + (vz - pltpu.roll(vz, 1, 0)))
        if ends:
            fresh = jnp.where(on, fresh, p)
        p = fresh
        for mask, (_, _, amounts) in zip(masks, points):
            p = p + jnp.where(mask, amounts[t], 0.0)
    return p, vr, vz


def pack_columns(load, lane, start, place):
    total = None
    for g in range(8):
        moved = pltpu.roll(load(g), (16 * g + place - start) % 128, 1)
        total = moved if total is None else jnp.where(lane >= 16 * g + place, moved, total)
    return total


def kernel(
    n_range, n_depth,
    p_in, vr_in, vz_in, c_in, rho_in, ac_in, ad_in, shifts, sources, wavelet,
    main, tail, strip,
    ext, beyond, raw, tail_out, edge_out, edge_in,
    in_sem, raw_sem, halo_send, halo_recv, far_send, far_recv, edge_send, edge_recv, tail_send, tail_recv,
):
    r = lax.axis_index("range")
    d = lax.axis_index("depth")
    height = p_in.shape[0]
    chunks = height // ROWS
    at_end = r == n_range - 1
    full = 128 * n_range
    span = ROWS + 2 * HALO

    barrier = pltpu.get_barrier_semaphore()

    @pl.when(r < n_range - 1)
    def _():
        pl.semaphore_signal(barrier, inc=1, device_id={"range": r + 1}, device_id_type=MESH)

    @pl.when(d > 0)
    def _():
        pl.semaphore_signal(barrier, inc=1, device_id={"depth": d - 1}, device_id_type=MESH)

    @pl.when(d < n_depth - 1)
    def _():
        pl.semaphore_signal(barrier, inc=1, device_id={"depth": d + 1}, device_id_type=MESH)

    loads = [
        pltpu.make_async_copy(ref, ext.at[i, pl.ds(HALO, height)], in_sem.at[i])
        for i, ref in enumerate((p_in, vr_in, vz_in, c_in, rho_in))
    ]
    for copy in loads:
        copy.start()
    far_loads = [
        pltpu.make_async_copy(ref, raw.at[i], raw_sem.at[i]) for i, ref in enumerate((ac_in, ad_in))
    ]

    @pl.when(at_end)
    def _():
        for copy in far_loads:
            copy.start()

    offsets = [jnp.int32(0)]
    for t in range(ITERS - 1):
        offsets.append(offsets[-1] + shifts[t])
    points = [
        (sources[i, 0], sources[i, 1], [wavelet[i, t] for t in range(ITERS)])
        for i in range(sources.shape[0])
    ]
    row_start = d * height
    iota_row = lax.broadcasted_iota(jnp.int32, (span, 128), 0)
    lane = lax.broadcasted_iota(jnp.int32, (span, 128), 1)
    col = lane + 128 * r

    for copy in loads:
        copy.wait()

    def pack_tail(i, results, target):
        half = ROWS // 2
        low = lane[:half] < TAIL
        for f, value in enumerate(results):
            first = value[HALO : HALO + half]
            second = pltpu.roll(value[HALO + half : HALO + ROWS], TAIL, 1)
            target[i, f] = jnp.where(low, first, second)

    def main_chunk(i):
        at = pl.multiple_of(i * ROWS, ROWS)
        fields = [ext[f, pl.ds(at, span)] for f in range(5)]
        row = iota_row + (row_start - HALO + at)
        results = advance(fields, row, col, offsets, points, full, True, False)
        for f, value in enumerate(results):
            main[f, pl.ds(at, ROWS)] = value[HALO : HALO + ROWS]
        pack_tail(i, results, tail_out)

    def tail_copy(i):
        return pltpu.make_async_remote_copy(
            src_ref=tail_out.at[i], dst_ref=tail.at[i],
            send_sem=tail_send.at[i], recv_sem=tail_recv.at[i],
            device_id={"range": r - 1}, device_id_type=MESH,
        )

    def send_tail(i):
        @pl.when(r > 0)
        def _():
            tail_copy(i).start()

    pl.semaphore_wait(
        barrier, jnp.minimum(r, 1) + jnp.minimum(d, 1) + jnp.minimum(n_depth - 1 - d, 1)
    )

    up = pltpu.make_async_remote_copy(
        src_ref=ext.at[:, pl.ds(HALO, HALO)], dst_ref=ext.at[:, pl.ds(HALO + height, HALO)],
        send_sem=halo_send.at[0], recv_sem=halo_recv.at[0],
        device_id={"depth": d - 1}, device_id_type=MESH,
    )
    down = pltpu.make_async_remote_copy(
        src_ref=ext.at[:, pl.ds(height, HALO)], dst_ref=ext.at[:, pl.ds(0, HALO)],
        send_sem=halo_send.at[1], recv_sem=halo_recv.at[1],
        device_id={"depth": d + 1}, device_id_type=MESH,
    )

    @pl.when(d > 0)
    def _():
        up.start()

    @pl.when(d < n_depth - 1)
    def _():
        down.start()

    zeros = jnp.zeros((HALO, 128), jnp.float32)

    @pl.when(d == 0)
    def _():
        for f in range(4):
            ext[f, pl.ds(0, HALO)] = zeros
        ext[4, pl.ds(0, HALO)] = zeros + 1.0

    @pl.when(d == n_depth - 1)
    def _():
        for f in range(4):
            ext[f, pl.ds(HALO + height, HALO)] = zeros
        last = ext[4, pl.ds(height, HALO)]
        ext[4, pl.ds(HALO + height, HALO)] = jnp.broadcast_to(last[HALO - 1 :], (HALO, 128))

    def interior(i, carry):
        main_chunk(i)
        send_tail(i)
        return carry

    lax.fori_loop(1, chunks - 1, interior, 0)

    @pl.when(d < n_depth - 1)
    def _():
        up.wait_recv()

    @pl.when(d > 0)
    def _():
        down.wait_recv()

    def rim(i, carry):
        main_chunk(i * (chunks - 1))
        send_tail(i * (chunks - 1))
        return carry

    lax.fori_loop(0, 2, rim, 0)

    fold = span // 2
    high = (lane % 16) >= 8
    edge_copy = pltpu.make_async_remote_copy(
        src_ref=edge_out, dst_ref=edge_in, send_sem=edge_send, recv_sem=edge_recv,
        device_id={"range": r - 1}, device_id_type=MESH,
    )

    @pl.when(r > 0)
    def _():
        for f in range(5):
            packed = pack_columns(lambda g: ext[f, pl.ds(g * ROWS, span)], lane, 0, 8)
            edge_out[f] = jnp.where(
                high[:fold], packed[:fold], pltpu.roll(packed[fold:], 120, 1)
            )
        edge_copy.start()

    @pl.when(at_end)
    def _():
        for copy in far_loads:
            copy.wait()
        for f, fill in enumerate((0.0, 1.0)):
            side = jnp.full((height, 64), fill, jnp.float32)
            beyond[f, pl.ds(HALO, height)] = jnp.concatenate([raw[f], side], 1)

        far_up = pltpu.make_async_remote_copy(
            src_ref=beyond.at[:, pl.ds(HALO, HALO)], dst_ref=beyond.at[:, pl.ds(HALO + height, HALO)],
            send_sem=far_send.at[0], recv_sem=far_recv.at[0],
            device_id={"depth": d - 1}, device_id_type=MESH,
        )
        far_down = pltpu.make_async_remote_copy(
            src_ref=beyond.at[:, pl.ds(height, HALO)], dst_ref=beyond.at[:, pl.ds(0, HALO)],
            send_sem=far_send.at[1], recv_sem=far_recv.at[1],
            device_id={"depth": d + 1}, device_id_type=MESH,
        )

        @pl.when(d > 0)
        def _():
            far_up.start()

        @pl.when(d < n_depth - 1)
        def _():
            far_down.start()

        @pl.when(d == 0)
        def _():
            beyond[0, pl.ds(0, HALO)] = zeros
            beyond[1, pl.ds(0, HALO)] = zeros + 1.0

        @pl.when(d == n_depth - 1)
        def _():
            beyond[0, pl.ds(HALO + height, HALO)] = zeros
            last = beyond[1, pl.ds(height, HALO)]
            beyond[1, pl.ds(HALO + height, HALO)] = jnp.broadcast_to(last[HALO - 1 :], (HALO, 128))

        @pl.when(d < n_depth - 1)
        def _():
            far_up.wait_recv()

        @pl.when(d > 0)
        def _():
            far_down.wait_recv()

        nothing = jnp.zeros((span, 128), jnp.float32)

        def far_chunk(i, carry):
            at = pl.multiple_of(i * ROWS, ROWS)
            fields = [nothing] * 3 + [beyond[f, pl.ds(at, span)] for f in range(2)]
            row = iota_row + (row_start - HALO + at)
            results = advance(fields, row, lane + full, offsets, [], full, False, True)
            pack_tail(i, results, tail)
            return carry

        lax.fori_loop(0, chunks, far_chunk, 0)
        for f in range(3):
            edge_in[f] = nothing[:fold]
        for f in range(2):
            packed = pack_columns(lambda g: beyond[f, pl.ds(g * ROWS, span)], lane, 0, 8)
            edge_in[3 + f] = jnp.where(
                high[:fold], packed[:fold], pltpu.roll(packed[fold:], 120, 1)
            )

        @pl.when(d > 0)
        def _():
            far_up.wait_send()

        @pl.when(d < n_depth - 1)
        def _():
            far_down.wait_send()

    own = [
        pack_columns(lambda g: ext[f, pl.ds(g * ROWS, span)], lane, 120, 0) for f in range(5)
    ]

    @pl.when(r < n_range - 1)
    def _():
        edge_copy.wait_recv()

    fields = []
    for f in range(5):
        folded = edge_in[f]
        other = jnp.concatenate([folded, pltpu.roll(folded, 8, 1)], 0)
        fields.append(jnp.where(high, other, own[f]))
    row = iota_row + (row_start - HALO) + ROWS * (lane // 16)
    results = advance(
        fields, row, 128 * r + 120 + lane % 16, offsets, points, full, False, True
    )
    for f, value in enumerate(results):
        strip[f] = value[HALO : HALO + ROWS]

    @pl.when(r < n_range - 1)
    def _():
        for i in range(chunks):
            tail_copy(i).wait_recv()

    @pl.when(r > 0)
    def _():
        edge_copy.wait_send()
        for i in range(chunks):
            tail_copy(i).wait_send()

    @pl.when(d > 0)
    def _():
        up.wait_send()

    @pl.when(d < n_depth - 1)
    def _():
        down.wait_send()


def finish(main, tail, strip, shifts, p_out, vr_out, vz_out, out, sem):
    chunks = tail.shape[0]
    offset = shifts[0]
    for t in range(1, ITERS):
        offset = offset + shifts[t]
    half = ROWS // 2
    lane = lax.broadcasted_iota(jnp.int32, (half, 128), 1)
    copies = []
    for i in range(chunks):
        for f, target in enumerate((p_out, vr_out, vz_out)):
            packed = tail[i, f]
            for h in range(2):
                at = i * ROWS + h * half
                edge = pltpu.roll(strip[f, h * half : (h + 1) * half], (120 - 16 * i) % 128, 1)
                near = jnp.where(lane >= 124, edge, main[f, at : at + half])
                far = packed if h == 0 else pltpu.roll(packed, TAIL, 1)
                far = jnp.where(lane < 4, edge, far)
                out[f, at : at + half] = pltpu.roll(
                    jnp.where(lane >= offset, near, far), 128 - offset, 1
                )
            copy = pltpu.make_async_copy(
                out.at[f, pl.ds(i * ROWS, ROWS)], target.at[pl.ds(i * ROWS, ROWS)], sem.at[i, f]
            )
            copy.start()
            copies.append(copy)
    for copy in copies:
        copy.wait()


def solution(mesh):
    n_range, n_depth = mesh.shape["range"], mesh.shape["depth"]

    def step(p, vr, vz, c, rho, ac, ad, shifts, sources, wavelet):
        height = p.shape[0]
        chunks = height // ROWS
        span = ROWS + 2 * HALO
        f32 = jnp.float32
        dma = pltpu.SemaphoreType.DMA
        any_space = pl.BlockSpec(memory_space=pl.ANY)
        vmem = pl.BlockSpec(memory_space=pltpu.VMEM)
        smem = pl.BlockSpec(memory_space=pltpu.SMEM)
        main, tail, strip = pl.pallas_call(
            functools.partial(kernel, n_range, n_depth),
            out_shape=(
                jax.ShapeDtypeStruct((3, height, 128), f32),
                jax.ShapeDtypeStruct((chunks, 3, ROWS // 2, 128), f32),
                jax.ShapeDtypeStruct((3, ROWS, 128), f32),
            ),
            in_specs=[any_space] * 7 + [smem] * 3,
            out_specs=(vmem, vmem, vmem),
            scratch_shapes=[
                pltpu.VMEM((5, height + 2 * HALO, 128), f32),
                pltpu.VMEM((2, height + 2 * HALO, 128), f32),
                pltpu.VMEM((2, height, 64), f32),
                pltpu.VMEM((chunks, 3, ROWS // 2, 128), f32),
                pltpu.VMEM((5, span // 2, 128), f32),
                pltpu.VMEM((5, span // 2, 128), f32),
                dma((5,)), dma((2,)), dma((2,)), dma((2,)), dma((2,)), dma((2,)),
                dma, dma, dma((chunks,)), dma((chunks,)),
            ],
            compiler_params=pltpu.CompilerParams(
                collective_id=1, has_side_effects=True, vmem_limit_bytes=32 * 2**20
            ),
        )(p, vr, vz, c, rho, ac, ad, shifts, sources, wavelet)
        block = jax.ShapeDtypeStruct((height, 128), f32)
        return pl.pallas_call(
            finish,
            out_shape=(block, block, block),
            in_specs=[vmem, vmem, vmem, smem],
            out_specs=(any_space, any_space, any_space),
            scratch_shapes=[pltpu.VMEM((3, height, 128), f32), dma((chunks, 3))],
            compiler_params=pltpu.CompilerParams(vmem_limit_bytes=16 * 2**20),
        )(main, tail, strip, shifts)

    block = P("depth", "range")
    return jax.shard_map(
        step,
        mesh=mesh,
        in_specs=(block,) * 5 + (P("depth", None),) * 2 + (P(),) * 3,
        out_specs=(block, block, block),
        check_vma=False,
    )
```

```python
import functools

import jax
import jax.numpy as jnp
from jax import lax
from jax.experimental import pallas as pl
from jax.experimental.pallas import tpu as pltpu
from jax.sharding import PartitionSpec as P

ITERS = 4
TIME_STEP = 0.6
MESH = pl.DeviceIdType.MESH
HALO = 8
ROWS = 128
TAIL = 64
RING = 8
FAR = 5


def advance(fields, row, col, offsets, points, full, left, ends):
    p, vr, vz, c, rho = fields
    n = p.shape[0]
    a = (2.0 * TIME_STEP) / (rho + pltpu.roll(rho, 127, 1))
    b = (2.0 * TIME_STEP) / (rho + pltpu.roll(rho, n - 1, 0))
    b = jnp.where(row >= 0, b, 0.0)
    k = TIME_STEP * (rho * c * c)
    if ends:
        a_last = TIME_STEP / rho
    masks = []
    for where_row, where_col, _ in points:
        masks.append(jnp.logical_and(row == where_row, col == where_col))
    for t in range(ITERS):
        push_r = pltpu.roll(p, 127, 1) - p
        push_z = b * (pltpu.roll(p, n - 1, 0) - p)
        if ends:
            on = col < full + offsets[t]
            push_r = jnp.where(col == full + offsets[t] - 1, a_last, a) * push_r
            vr = jnp.where(on, vr - push_r, vr)
            vz = jnp.where(on, vz - push_z, vz)
        else:
            vr = vr - a * push_r
            vz = vz - push_z
        back = pltpu.roll(vr, 1, 1)
        if left:
            back = jnp.where(col == offsets[t], 0.0, back)
        fresh = p - k * ((vr - back) + (vz - pltpu.roll(vz, 1, 0)))
        if ends:
            fresh = jnp.where(on, fresh, p)
        p = fresh
        for mask, (_, _, amounts) in zip(masks, points):
            p = p + jnp.where(mask, amounts[t], 0.0)
    return p, vr, vz


def pack_columns(load, lane, start, place):
    total = None
    for g in range(8):
        moved = pltpu.roll(load(g), (16 * g + place - start) % 128, 1)
        total = moved if total is None else jnp.where(lane >= 16 * g + place, moved, total)
    return total


def kernel(
    n_range, n_depth,
    p_in, vr_in, vz_in, c_in, rho_in, ac_in, ad_in, shifts, sources, wavelet,
    main, tail, strip,
    ext, beyond, raw, tail_out, edge_out, edge_in, relay, relay_edge, seam, main_out, strip_out,
    in_sem, raw_sem, halo_send, halo_recv, far_send, far_recv, edge_send, edge_recv, tail_send, tail_recv,
    pass_send, pass_recv, edge_pass_send, edge_pass_recv, ready_wrap, ready_next, main_sem, strip_sem,
):
    r = lax.axis_index("range")
    d = lax.axis_index("depth")
    z = lax.rem(r, RING)
    height = p_in.shape[0]
    chunks = height // ROWS
    at_end = r == n_range - 1
    full = 128 * n_range
    span = ROWS + 2 * HALO
    half = ROWS // 2
    quarter = ROWS // 4

    seam_out = jnp.logical_and(z == 0, r > 0)
    seam_in = jnp.logical_and(z == RING - 1, r < n_range - 1)
    upper = r >= RING
    lower = r < n_range - RING
    base = jnp.logical_and(z == 0, lower)
    first_stop = jnp.logical_and(jnp.logical_and(z >= 1, z <= 3), upper)
    second_stop = jnp.logical_and(jnp.logical_and(z >= 4, z <= 6), lower)
    plain_out = z > 0
    plain_in = z < RING - 1

    def one(flag):
        return jnp.where(flag, 1, 0)

    barrier = pltpu.get_barrier_semaphore()

    def greet(flag, semaphore, **where):
        @pl.when(flag)
        def _():
            pl.semaphore_signal(semaphore, inc=1, device_id=where, device_id_type=MESH)

    greet(plain_in, barrier, range=r + 1)
    greet(base, barrier, range=r + RING)
    greet(base, barrier, range=r + RING - 1)
    greet(seam_out, barrier, range=r + 2)
    greet(seam_out, barrier, range=r + 3)
    greet(first_stop, barrier, range=r - RING + 3)
    greet(jnp.logical_and(z == 4, lower), barrier, range=r + 3)
    greet(jnp.logical_and(z == 5, lower), barrier, range=r + 2)
    greet(d > 0, barrier, depth=d - 1)
    greet(d < n_depth - 1, barrier, depth=d + 1)

    loads = [
        pltpu.make_async_copy(ref, ext.at[i, pl.ds(HALO, height)], in_sem.at[i])
        for i, ref in enumerate((p_in, vr_in, vz_in, c_in, rho_in))
    ]
    for copy in loads:
        copy.start()
    far_loads = [
        pltpu.make_async_copy(ref, raw.at[i], raw_sem.at[i]) for i, ref in enumerate((ac_in, ad_in))
    ]

    @pl.when(at_end)
    def _():
        for copy in far_loads:
            copy.start()

    offsets = [jnp.int32(0)]
    for t in range(ITERS - 1):
        offsets.append(offsets[-1] + shifts[t])
    points = [
        (sources[0, i], sources[1, i], [wavelet[t, i] for t in range(ITERS)])
        for i in range(sources.shape[1])
    ]
    row_start = d * height
    iota_row = lax.broadcasted_iota(jnp.int32, (span, 128), 0)
    lane = lax.broadcasted_iota(jnp.int32, (span, 128), 1)
    col = lane + 128 * r

    for copy in loads:
        copy.wait()

    def pack_tail(i, results, target):
        low = lane[:half] < TAIL
        for f, value in enumerate(results):
            first = value[HALO : HALO + half]
            second = pltpu.roll(value[HALO + half : HALO + ROWS], TAIL, 1)
            target[i, f] = jnp.where(low, first, second)

    def main_copy(i):
        at = pl.ds(pl.multiple_of(i * ROWS, ROWS), ROWS)
        return pltpu.make_async_copy(main_out.at[:, at], main.at[:, at], main_sem.at[i])

    def main_chunk(i):
        at = pl.multiple_of(i * ROWS, ROWS)
        fields = [ext[f, pl.ds(at, span)] for f in range(5)]
        row = iota_row + (row_start - HALO + at)
        results = advance(fields, row, col, offsets, points, full, True, False)
        for f, value in enumerate(results):
            main_out[f, pl.ds(at, ROWS)] = value[HALO : HALO + ROWS]
        pack_tail(i, results, tail_out)
        main_copy(i).start()

    def remote(src, dst, send, recv, **where):
        return pltpu.make_async_remote_copy(
            src_ref=src, dst_ref=dst, send_sem=send, recv_sem=recv,
            device_id=where, device_id_type=MESH,
        )

    def tail_copy(i):
        return remote(tail_out.at[i], tail.at[i], tail_send.at[i], tail_recv.at[i], range=r - 1)

    def low_copy(i):
        return remote(tail_out.at[i], relay.at[i], tail_send.at[i], pass_recv.at[i, 0], range=r - RING)

    def wrap_copy(i):
        return remote(relay.at[i], tail.at[i], pass_send.at[i, 0], tail_recv.at[i], range=r + RING - 1)

    def part(ref, i, j):
        return ref.at[i, :, pl.ds(j * quarter, quarter)]

    def hop(i, j, source, target, to):
        return remote(part(source, i, j), part(target, i, j), pass_send.at[i, j], pass_recv.at[i, j], range=to)

    def edge_hop(f, source, target, to):
        return remote(source.at[f], target.at[f], edge_pass_send.at[f], edge_pass_recv.at[f], range=to)

    edge_copy = remote(edge_out, edge_in, edge_send, edge_recv, range=r - 1)

    pl.semaphore_wait(
        barrier,
        one(plain_out) + one(seam_out) + 3 * one(seam_in) + one(second_stop)
        + one(jnp.logical_and(first_stop, z >= 2))
        + one(d > 0) + one(d < n_depth - 1),
    )

    up = remote(
        ext.at[:, pl.ds(HALO, HALO)], ext.at[:, pl.ds(HALO + height, HALO)],
        halo_send.at[0], halo_recv.at[0], depth=d - 1,
    )
    down = remote(
        ext.at[:, pl.ds(height, HALO)], ext.at[:, pl.ds(0, HALO)],
        halo_send.at[1], halo_recv.at[1], depth=d + 1,
    )

    @pl.when(d > 0)
    def _():
        up.start()

    @pl.when(d < n_depth - 1)
    def _():
        down.start()

    greet(seam_in, ready_wrap, range=r - RING + 1)
    for t in (1, 2, 3):
        greet(jnp.logical_and(first_stop, z == t), ready_next.at[t - 1], range=r - t)
        greet(seam_in, ready_next.at[0], range=r - t)
    greet(second_stop, ready_next.at[0], range=r + RING - 3)

    zeros = jnp.zeros((HALO, 128), jnp.float32)

    @pl.when(d == 0)
    def _():
        for f in range(4):
            ext[f, pl.ds(0, HALO)] = zeros
        ext[4, pl.ds(0, HALO)] = zeros + 1.0

    @pl.when(d == n_depth - 1)
    def _():
        for f in range(4):
            ext[f, pl.ds(HALO + height, HALO)] = zeros
        last = ext[4, pl.ds(height, HALO)]
        ext[4, pl.ds(HALO + height, HALO)] = jnp.broadcast_to(last[HALO - 1 :], (HALO, 128))

    def interior(i, carry):
        main_chunk(i)

        @pl.when(plain_out)
        def _():
            tail_copy(i).start()

        @pl.when(jnp.logical_and(seam_out, i > FAR))
        def _():
            low_copy(i).start()

        @pl.when(jnp.logical_and(seam_out, i <= 2))
        def _():
            @pl.when(i == 1)
            def _():
                pl.semaphore_wait(ready_next.at[0], 1)

            for j in range(2):
                hop(i, j, tail_out, relay, r + 1).start()

        @pl.when(jnp.logical_and(seam_out, jnp.logical_and(i >= 3, i <= FAR)))
        def _():
            @pl.when(i == 3)
            def _():
                pl.semaphore_wait(ready_next.at[1], 1)

            for j in range(2):
                hop(i, j, tail_out, relay, r + 2).start()

        return carry

    lax.fori_loop(1, 4, interior, 0)

    @pl.when(d < n_depth - 1)
    def _():
        up.wait_recv()

    @pl.when(d > 0)
    def _():
        down.wait_recv()

    fold = span // 2
    high = (lane % 16) >= 8

    def fold_edge(load, target, first):
        def body(f, carry):
            packed = pack_columns(lambda g: load(f, g), lane, 0, 8)
            target[f + first] = jnp.where(high[:fold], packed[:fold], pltpu.roll(packed[fold:], 120, 1))
            return carry

        return body

    @pl.when(r > 0)
    def _():
        lax.fori_loop(0, 5, fold_edge(lambda f, g: ext[f, pl.ds(g * ROWS, span)], edge_out, 0), 0)

    @pl.when(plain_out)
    def _():
        edge_copy.start()

    @pl.when(seam_out)
    def _():
        pl.semaphore_wait(ready_next.at[2], 1)
        for f in range(5):
            edge_hop(f, edge_out, relay_edge, r + 3).start()

    lax.fori_loop(4, chunks - 1, interior, 0)

    def rim(i, carry):
        main_chunk(i * (chunks - 1))

        @pl.when(plain_out)
        def _():
            tail_copy(i * (chunks - 1)).start()

        @pl.when(seam_out)
        def _():
            low_copy(i * (chunks - 1)).start()

        return carry

    lax.fori_loop(0, 2, rim, 0)

    @pl.when(at_end)
    def _():
        for copy in far_loads:
            copy.wait()

        def turn_block(i, carry):
            at = pl.multiple_of(i * ROWS, ROWS)
            for f, fill in enumerate((0.0, 1.0)):
                block = raw[f, :, pl.ds(at, ROWS)]
                block = jnp.concatenate([block, jnp.full((128 - TAIL, ROWS), fill, jnp.float32)], 0)
                beyond[f, pl.ds(HALO + at, ROWS)] = block.T
            return carry

        lax.fori_loop(0, chunks, turn_block, 0)
        far_up = remote(
            beyond.at[:, pl.ds(HALO, HALO)], beyond.at[:, pl.ds(HALO + height, HALO)],
            far_send.at[0], far_recv.at[0], depth=d - 1,
        )
        far_down = remote(
            beyond.at[:, pl.ds(height, HALO)], beyond.at[:, pl.ds(0, HALO)],
            far_send.at[1], far_recv.at[1], depth=d + 1,
        )

        @pl.when(d > 0)
        def _():
            far_up.start()

        @pl.when(d < n_depth - 1)
        def _():
            far_down.start()

        @pl.when(d == 0)
        def _():
            beyond[0, pl.ds(0, HALO)] = zeros
            beyond[1, pl.ds(0, HALO)] = zeros + 1.0

        @pl.when(d == n_depth - 1)
        def _():
            beyond[0, pl.ds(HALO + height, HALO)] = zeros
            last = beyond[1, pl.ds(height, HALO)]
            beyond[1, pl.ds(HALO + height, HALO)] = jnp.broadcast_to(last[HALO - 1 :], (HALO, 128))

        @pl.when(d < n_depth - 1)
        def _():
            far_up.wait_recv()

        @pl.when(d > 0)
        def _():
            far_down.wait_recv()

        nothing = jnp.zeros((span, 128), jnp.float32)

        def far_out(i):
            return pltpu.make_async_copy(relay.at[i], tail.at[i], pass_send.at[i, 0])

        def far_chunk(i, carry):
            at = pl.multiple_of(i * ROWS, ROWS)
            fields = [nothing] * 3 + [beyond[f, pl.ds(at, span)] for f in range(2)]
            row = iota_row + (row_start - HALO + at)
            results = advance(fields, row, lane + full, offsets, [], full, False, True)
            pack_tail(i, results, relay)
            far_out(i).start()
            return carry

        lax.fori_loop(0, chunks, far_chunk, 0)
        for i in range(chunks):
            far_out(i).wait()
        for f in range(3):
            edge_in[f] = nothing[:fold]
        lax.fori_loop(0, 2, fold_edge(lambda f, g: beyond[f, pl.ds(g * ROWS, span)], edge_in, 3), 0)

        @pl.when(d > 0)
        def _():
            far_up.wait_send()

        @pl.when(d < n_depth - 1)
        def _():
            far_down.wait_send()

    near = [i for i in range(chunks) if not 1 <= i <= FAR]

    @pl.when(base)
    def _():
        pl.semaphore_wait(ready_wrap, 1)
        for i in near[1:-1] + [near[0], near[-1]]:
            low_copy(i).wait_recv()
            wrap_copy(i).start()

    leg = jnp.where(z >= 4, z - 3, z)
    first_chunk = jnp.where(leg == 1, 1, 3)
    last_chunk = jnp.where(leg == 1, 3, jnp.where(leg == 2, FAR + 1, 3))
    to = jnp.where(first_stop, r - RING + 3, r + RING - 1 - z)
    passes = jnp.logical_or(first_stop, second_stop)

    @pl.when(passes)
    def _():
        pl.semaphore_wait(ready_next.at[0], 1)

        def pass_on(i, carry):
            for j in range(2):
                hop(i, j, relay, relay, to).wait_recv()

                @pl.when(first_stop)
                def _():
                    hop(i, j, relay, relay, to).start()

                @pl.when(second_stop)
                def _():
                    hop(i, j, relay, tail, to).start()

            return carry

        lax.fori_loop(first_chunk, last_chunk, pass_on, 0)

        @pl.when(leg == 3)
        def _():
            for f in range(5):
                edge_hop(f, relay_edge, relay_edge, to).wait_recv()

                @pl.when(first_stop)
                def _():
                    edge_hop(f, relay_edge, relay_edge, to).start()

                @pl.when(second_stop)
                def _():
                    edge_hop(f, relay_edge, edge_in, to).start()

    @pl.when(plain_in)
    def _():
        edge_copy.wait_recv()

    @pl.when(seam_in)
    def _():
        for f in range(5):
            edge_hop(f, relay_edge, edge_in, r).wait_recv()

    def own_edge(f, carry):
        packed = pack_columns(lambda g: ext[f, pl.ds(g * ROWS, span)], lane, 120, 0)
        folded = edge_in[f]
        other = jnp.concatenate([folded, pltpu.roll(folded, 8, 1)], 0)
        seam[f] = jnp.where(high, other, packed)
        return carry

    lax.fori_loop(0, 5, own_edge, 0)
    row = iota_row + (row_start - HALO) + ROWS * (lane // 16)
    results = advance(
        [seam[f] for f in range(5)], row, 128 * r + 120 + lane % 16, offsets, points, full, False, True
    )
    for f, value in enumerate(results):
        strip_out[f] = value[HALO : HALO + ROWS]
    strip_copy = pltpu.make_async_copy(strip_out, strip, strip_sem)
    strip_copy.start()

    @pl.when(plain_in)
    def _():
        for i in range(chunks):
            tail_copy(i).wait_recv()

    @pl.when(seam_in)
    def _():
        for i in near:
            tail_copy(i).wait_recv()
        for i in range(1, FAR + 1):
            for j in range(2):
                hop(i, j, relay, tail, r).wait_recv()

    @pl.when(plain_out)
    def _():
        edge_copy.wait_send()
        for i in range(chunks):
            tail_copy(i).wait_send()

    @pl.when(seam_out)
    def _():
        for i in near:
            low_copy(i).wait_send()
        for i in range(1, FAR + 1):
            for j in range(2):
                hop(i, j, tail_out, relay, r).wait_send()
        for f in range(5):
            edge_hop(f, edge_out, relay_edge, r).wait_send()

    @pl.when(base)
    def _():
        for i in near:
            wrap_copy(i).wait_send()

    @pl.when(passes)
    def _():
        def passed(i, carry):
            for j in range(2):
                hop(i, j, relay, relay, r).wait_send()
            return carry

        lax.fori_loop(first_chunk, last_chunk, passed, 0)

        @pl.when(leg == 3)
        def _():
            for f in range(5):
                edge_hop(f, relay_edge, relay_edge, r).wait_send()

    strip_copy.wait()
    for i in range(chunks):
        main_copy(i).wait()

    @pl.when(d > 0)
    def _():
        up.wait_send()

    @pl.when(d < n_depth - 1)
    def _():
        down.wait_send()


def finish(main_in, tail_in, strip_in, shifts, p_out, vr_out, vz_out, main, tail, strip, out, in_sem, strip_sem, sem):
    chunks = tail.shape[0]

    def rows(i):
        return pl.ds(pl.multiple_of(i * ROWS, ROWS), ROWS)

    strip_copy = pltpu.make_async_copy(strip_in, strip, strip_sem)
    strip_copy.start()

    def loads(i):
        return (
            pltpu.make_async_copy(main_in.at[:, rows(i)], main.at[:, rows(i)], in_sem.at[i, 0]),
            pltpu.make_async_copy(tail_in.at[i], tail.at[i], in_sem.at[i, 1]),
        )

    for i in range(chunks):
        for copy in loads(i):
            copy.start()
    offset = shifts[0]
    for t in range(1, ITERS):
        offset = offset + shifts[t]
    half = ROWS // 2
    lane = lax.broadcasted_iota(jnp.int32, (half, 128), 1)
    outs = (p_out, vr_out, vz_out)

    def store(i, f):
        return pltpu.make_async_copy(out.at[f, rows(i)], outs[f].at[rows(i)], sem.at[i, f])

    strip_copy.wait()

    def body(i, carry):
        for copy in loads(i):
            copy.wait()
        for f in range(3):
            packed = tail[i, f]
            for h in range(2):
                at = pl.ds(pl.multiple_of(i * ROWS + h * half, half), half)
                edge = pltpu.roll(strip[f, h * half : (h + 1) * half], 248 - 16 * i, 1)
                near = jnp.where(lane >= 124, edge, main[f, at])
                far = packed if h == 0 else pltpu.roll(packed, TAIL, 1)
                far = jnp.where(lane < 4, edge, far)
                out[f, at] = pltpu.roll(jnp.where(lane >= offset, near, far), 128 - offset, 1)
            store(i, f).start()
        return carry

    lax.fori_loop(0, chunks, body, 0)
    for i in range(chunks):
        for f in range(3):
            store(i, f).wait()


def solution(mesh):
    n_range, n_depth = mesh.shape["range"], mesh.shape["depth"]

    def step(p, vr, vz, c, rho, ac, ad, shifts, sources, wavelet):
        height = p.shape[0]
        chunks = height // ROWS
        span = ROWS + 2 * HALO
        f32 = jnp.float32
        dma = pltpu.SemaphoreType.DMA
        hbm = pl.BlockSpec(memory_space=pltpu.HBM)
        smem = pl.BlockSpec(memory_space=pltpu.SMEM)
        main, tail, strip = pl.pallas_call(
            functools.partial(kernel, n_range, n_depth),
            out_shape=(
                jax.ShapeDtypeStruct((3, height, 128), f32),
                jax.ShapeDtypeStruct((chunks, 3, ROWS // 2, 128), f32),
                jax.ShapeDtypeStruct((3, ROWS, 128), f32),
            ),
            in_specs=[hbm] * 7 + [smem] * 3,
            out_specs=(hbm, hbm, hbm),
            scratch_shapes=[
                pltpu.VMEM((5, height + 2 * HALO, 128), f32),
                pltpu.VMEM((2, height + 2 * HALO, 128), f32),
                pltpu.VMEM((2, 64, height), f32),
                pltpu.VMEM((chunks, 3, ROWS // 2, 128), f32),
                pltpu.VMEM((5, span // 2, 128), f32),
                pltpu.VMEM((5, span // 2, 128), f32),
                pltpu.VMEM((chunks, 3, ROWS // 2, 128), f32),
                pltpu.VMEM((5, span // 2, 128), f32),
                pltpu.VMEM((5, span, 128), f32),
                pltpu.VMEM((3, height, 128), f32),
                pltpu.VMEM((3, ROWS, 128), f32),
                dma((5,)), dma((2,)), dma((2,)), dma((2,)), dma((2,)), dma((2,)),
                dma, dma, dma((chunks,)), dma((chunks,)), dma((chunks, 2)), dma((chunks, 2)), dma((5,)), dma((5,)),
                pltpu.SemaphoreType.REGULAR, pltpu.SemaphoreType.REGULAR((3,)), dma((chunks,)), dma,
            ],
            compiler_params=pltpu.CompilerParams(
                collective_id=1, has_side_effects=True, vmem_limit_bytes=58 * 2**20
            ),
        )(p, vr, vz, c, rho, ac.T, ad.T, shifts, sources.T, wavelet.T)
        block = jax.ShapeDtypeStruct((height, 128), f32)
        return pl.pallas_call(
            finish,
            out_shape=(block, block, block),
            in_specs=[hbm, hbm, hbm, smem],
            out_specs=(hbm, hbm, hbm),
            scratch_shapes=[
                pltpu.VMEM((3, height, 128), f32),
                pltpu.VMEM((chunks, 3, ROWS // 2, 128), f32),
                pltpu.VMEM((3, ROWS, 128), f32),
                pltpu.VMEM((3, height, 128), f32),
                dma((chunks, 2)), dma, dma((chunks, 3)),
            ],
            compiler_params=pltpu.CompilerParams(vmem_limit_bytes=58 * 2**20),
        )(main, tail, strip, shifts)

    block = P("depth", "range")
    return jax.shard_map(
        step,
        mesh=mesh,
        in_specs=(block,) * 5 + (P("depth", None),) * 2 + (P(),) * 3,
        out_specs=(block, block, block),
        check_vma=False,
    )
```

```python
import functools

import jax
import jax.numpy as jnp
from jax import lax
from jax.experimental import pallas as pl
from jax.experimental.pallas import tpu as pltpu
from jax.sharding import PartitionSpec as P

ITERS = 4
TIME_STEP = 0.6
MESH = pl.DeviceIdType.MESH
HALO = 8
ROWS = 128
WIDTHS = (40, 48, 64)
AHEAD = 64
RING = 8
FAR = 5


def advance(fields, row, col, offsets, inject, full, left, ends):
    p, vr, vz, c, rho = fields
    n = p.shape[0]
    a = (2.0 * TIME_STEP) / (rho + pltpu.roll(rho, 127, 1))
    b = (2.0 * TIME_STEP) / (rho + pltpu.roll(rho, n - 1, 0))
    b = jnp.where(row >= 0, b, 0.0)
    k = TIME_STEP * (rho * c * c)
    if ends:
        a_last = TIME_STEP / rho
    for t in range(ITERS):
        push_r = pltpu.roll(p, 127, 1) - p
        push_z = b * (pltpu.roll(p, n - 1, 0) - p)
        if ends:
            on = col < full + offsets[t]
            push_r = jnp.where(col == full + offsets[t] - 1, a_last, a) * push_r
            vr = jnp.where(on, vr - push_r, vr)
            vz = jnp.where(on, vz - push_z, vz)
        else:
            vr = vr - a * push_r
            vz = vz - push_z
        back = pltpu.roll(vr, 1, 1)
        if left:
            back = jnp.where(col == offsets[t], 0.0, back)
        fresh = p - k * ((vr - back) + (vz - pltpu.roll(vz, 1, 0)))
        if ends:
            fresh = jnp.where(on, fresh, p)
        p = fresh
        if inject is not None:
            p = p + inject(t)
    return p, vr, vz


def pack_columns(load, lane, start, place):
    total = None
    for g in range(8):
        moved = pltpu.roll(load(g), (16 * g + place - start) % 128, 1)
        total = moved if total is None else jnp.where(lane >= 16 * g + place, moved, total)
    return total


def pieces(width):
    found, end, first = [], 128, 0
    for lanes in (64, 32, 16, 8):
        if width - first >= lanes:
            found.append((lanes, end, first))
            end, first = end - lanes, first + lanes
    return found


def pack(value, width, lane):
    parts = []
    for lanes, end, _ in pieces(width):
        total = None
        for q in range(ROWS // lanes):
            moved = pltpu.roll(value[lanes * q : lanes * (q + 1)], (128 - end - lanes * q) % 128, 1)
            total = moved if q == 0 else jnp.where(lane[:lanes] < 128 - lanes * q, moved, total)
        parts.append(total)
    return parts[0] if len(parts) == 1 else jnp.concatenate(parts, 0)


def unpack(value, width, lane):
    result = None
    for lanes, end, first in reversed(pieces(width)):
        block = value[first : first + lanes]
        rows = [
            pltpu.roll(block, (lanes * q + end) % 128, 1) for q in range(ROWS // lanes)
        ]
        spread = jnp.concatenate(rows, 0)
        result = spread if result is None else jnp.where(lane >= end - lanes, spread, result)
    return result


def kernel(
    width, n_range, n_depth,
    p_in, vr_in, vz_in, c_in, rho_in, ac_in, ad_in, shifts, sources, wavelet,
    main, tail,
    ext, beyond, raw, tail_out, edge_out, edge_in, relay, relay_edge, seam, strip, spread,
    in_sem, raw_sem, halo_send, halo_recv, far_send, far_recv, edge_send, edge_recv, tail_send, tail_recv,
    pass_send, pass_recv, edge_pass_send, edge_pass_recv, ready_wrap, ready_next,
):
    r = lax.axis_index("range")
    d = lax.axis_index("depth")
    z = lax.rem(r, RING)
    height = p_in.shape[0]
    chunks = height // ROWS
    at_end = r == n_range - 1
    full = 128 * n_range
    span = ROWS + 2 * HALO
    half = ROWS // 2

    seam_out = jnp.logical_and(z == 0, r > 0)
    seam_in = jnp.logical_and(z == RING - 1, r < n_range - 1)
    upper = r >= RING
    lower = r < n_range - RING
    base = jnp.logical_and(z == 0, lower)
    first_stop = jnp.logical_and(jnp.logical_and(z >= 1, z <= 3), upper)
    second_stop = jnp.logical_and(jnp.logical_and(z >= 4, z <= 6), lower)
    plain_out = z > 0
    plain_in = z < RING - 1

    def one(flag):
        return jnp.where(flag, 1, 0)

    barrier = pltpu.get_barrier_semaphore()

    def greet(flag, semaphore, **where):
        @pl.when(flag)
        def _():
            pl.semaphore_signal(semaphore, inc=1, device_id=where, device_id_type=MESH)

    greet(plain_in, barrier, range=r + 1)
    greet(base, barrier, range=r + RING)
    greet(base, barrier, range=r + RING - 1)
    greet(seam_out, barrier, range=r + 2)
    greet(seam_out, barrier, range=r + 3)
    greet(first_stop, barrier, range=r - RING + 3)
    greet(jnp.logical_and(z == 4, lower), barrier, range=r + 3)
    greet(jnp.logical_and(z == 5, lower), barrier, range=r + 2)
    greet(d > 0, barrier, depth=d - 1)
    greet(d < n_depth - 1, barrier, depth=d + 1)

    loads = [
        pltpu.make_async_copy(ref, ext.at[i, pl.ds(HALO, height)], in_sem.at[i])
        for i, ref in enumerate((p_in, vr_in, vz_in, c_in, rho_in))
    ]
    for copy in loads:
        copy.start()
    far_loads = [
        pltpu.make_async_copy(ref, raw.at[i], raw_sem.at[i]) for i, ref in enumerate((ac_in, ad_in))
    ]

    @pl.when(at_end)
    def _():
        for copy in far_loads:
            copy.start()

    offsets = [jnp.int32(0)]
    for t in range(ITERS):
        offsets.append(offsets[-1] + shifts[t])
    whole = offsets[-1]
    points = [
        (sources[0, i], sources[1, i], [wavelet[t, i] for t in range(ITERS)])
        for i in range(sources.shape[1])
    ]
    row_start = d * height
    iota_row = lax.broadcasted_iota(jnp.int32, (span, 128), 0)
    lane = lax.broadcasted_iota(jnp.int32, (span, 128), 1)
    col = lane + 128 * r

    narrow = jnp.bfloat16
    small_lane, small_row = lane[:8], iota_row[:8]
    source_row = jnp.full((8, 128), -HALO - 1, jnp.int32)
    for i, (where_row, _, _) in enumerate(points):
        source_row = jnp.where(
            jnp.logical_and(small_lane % 8 == i, small_lane < 24), where_row, source_row
        )
    source_row = jnp.broadcast_to(source_row[:1], (span, 128))
    for t in range(ITERS):
        amount = jnp.zeros((8, 128), jnp.float32)
        for i, (_, where_col, amounts) in enumerate(points):
            here = jnp.logical_and(small_row == i, small_lane + 128 * r == where_col)
            amount = jnp.where(here, amounts[t], amount)
        first = amount.astype(narrow).astype(jnp.float32)
        second = (amount - first).astype(narrow).astype(jnp.float32)
        third = amount - first - second
        spread[t] = jnp.concatenate(
            [first, second, third, jnp.zeros((104, 128), jnp.float32)], 0
        ).astype(narrow)

    def injector(row):
        picks = jnp.where(row == source_row, 1.0, 0.0).astype(narrow)
        return lambda t: jnp.dot(picks, spread[t], preferred_element_type=jnp.float32)

    for copy in loads:
        copy.wait()

    def rolled(value):
        return pltpu.roll(value[HALO : HALO + ROWS], 128 - whole, 1)

    def main_chunk(i):
        at = pl.multiple_of(i * ROWS, ROWS)
        fields = [ext[f, pl.ds(at, span)] for f in range(5)]
        row = iota_row + (row_start - HALO + at)
        results = advance(fields, row, col, offsets, injector(row), full, True, False)
        for f, value in enumerate(results):
            value = rolled(value)
            main[f, pl.ds(at, ROWS)] = value
            tail_out[i, f, pl.ds(0, width)] = pack(value, width, lane)

    def remote(src, dst, send, recv, **where):
        return pltpu.make_async_remote_copy(
            src_ref=src, dst_ref=dst, send_sem=send, recv_sem=recv,
            device_id=where, device_id_type=MESH,
        )

    def body(ref, i):
        return ref.at[i, :, pl.ds(0, width)]

    def tail_copy(i):
        return remote(body(tail_out, i), body(tail, i), tail_send.at[i], tail_recv.at[i], range=r - 1)

    def low_copy(i):
        return remote(body(tail_out, i), body(relay, i), tail_send.at[i], pass_recv.at[i, 0], range=r - RING)

    def wrap_copy(i):
        return remote(body(relay, i), body(tail, i), pass_send.at[i, 0], tail_recv.at[i], range=r + RING - 1)

    def part(ref, i, j):
        return ref.at[i, j, pl.ds(0, width)]

    def hop(i, j, source, target, to):
        return remote(part(source, i, j), part(target, i, j), pass_send.at[i, j], pass_recv.at[i, j], range=to)

    def edge_hop(f, source, target, to):
        return remote(source.at[f], target.at[f], edge_pass_send.at[f], edge_pass_recv.at[f], range=to)

    edge_copy = remote(edge_out, edge_in, edge_send, edge_recv, range=r - 1)

    pl.semaphore_wait(
        barrier,
        one(plain_out) + one(seam_out) + 3 * one(seam_in) + one(second_stop)
        + one(jnp.logical_and(first_stop, z >= 2))
        + one(d > 0) + one(d < n_depth - 1),
    )

    up = remote(
        ext.at[:, pl.ds(HALO, HALO)], ext.at[:, pl.ds(HALO + height, HALO)],
        halo_send.at[0], halo_recv.at[0], depth=d - 1,
    )
    down = remote(
        ext.at[:, pl.ds(height, HALO)], ext.at[:, pl.ds(0, HALO)],
        halo_send.at[1], halo_recv.at[1], depth=d + 1,
    )

    @pl.when(d > 0)
    def _():
        up.start()

    @pl.when(d < n_depth - 1)
    def _():
        down.start()

    greet(seam_in, ready_wrap, range=r - RING + 1)
    for t in (1, 2, 3):
        greet(jnp.logical_and(first_stop, z == t), ready_next.at[t - 1], range=r - t)
        greet(seam_in, ready_next.at[0], range=r - t)
    greet(second_stop, ready_next.at[0], range=r + RING - 3)

    zeros = jnp.zeros((HALO, 128), jnp.float32)

    @pl.when(d == 0)
    def _():
        for f in range(4):
            ext[f, pl.ds(0, HALO)] = zeros
        ext[4, pl.ds(0, HALO)] = zeros + 1.0

    @pl.when(d == n_depth - 1)
    def _():
        for f in range(4):
            ext[f, pl.ds(HALO + height, HALO)] = zeros
        last = ext[4, pl.ds(height, HALO)]
        ext[4, pl.ds(HALO + height, HALO)] = jnp.broadcast_to(last[HALO - 1 :], (HALO, 128))

    far_up = remote(
        beyond.at[:, pl.ds(HALO, HALO)], beyond.at[:, pl.ds(HALO + height, HALO)],
        far_send.at[0], far_recv.at[0], depth=d - 1,
    )
    far_down = remote(
        beyond.at[:, pl.ds(height, HALO)], beyond.at[:, pl.ds(0, HALO)],
        far_send.at[1], far_recv.at[1], depth=d + 1,
    )


    @pl.when(at_end)
    def _():
        for copy in far_loads:
            copy.wait()

        def turn_block(i, carry):
            at = pl.multiple_of(i * ROWS, ROWS)
            for f, fill in enumerate((0.0, 1.0)):
                block = raw[f, :, pl.ds(at, ROWS)]
                block = jnp.concatenate([block, jnp.full((128 - AHEAD, ROWS), fill, jnp.float32)], 0)
                beyond[f, pl.ds(HALO + at, ROWS)] = block.T
            return carry

        lax.fori_loop(0, chunks, turn_block, 0)
        @pl.when(d > 0)
        def _():
            far_up.start()

        @pl.when(d < n_depth - 1)
        def _():
            far_down.start()

        @pl.when(d == 0)
        def _():
            beyond[0, pl.ds(0, HALO)] = zeros
            beyond[1, pl.ds(0, HALO)] = zeros + 1.0

        @pl.when(d == n_depth - 1)
        def _():
            beyond[0, pl.ds(HALO + height, HALO)] = zeros
            last = beyond[1, pl.ds(height, HALO)]
            beyond[1, pl.ds(HALO + height, HALO)] = jnp.broadcast_to(last[HALO - 1 :], (HALO, 128))

    leg = jnp.where(z >= 4, z - 3, z)
    first_chunk = jnp.where(leg == 1, 1, 4)
    last_chunk = jnp.where(leg == 1, 4, jnp.where(leg == 2, FAR + 1, 4))
    to = jnp.where(first_stop, r - RING + 3, r + RING - 1 - z)
    passes = jnp.logical_or(first_stop, second_stop)

    def pass_on(i, carry):
        for j in range(3):
            hop(i, j, relay, relay, to).wait_recv()

            @pl.when(first_stop)
            def _():
                hop(i, j, relay, relay, to).start()

            @pl.when(second_stop)
            def _():
                hop(i, j, relay, tail, to).start()

        return carry

    def pass_chunks():
        lax.fori_loop(first_chunk, last_chunk, pass_on, 0)

    def pass_edge():
        for f in range(5):
            edge_hop(f, relay_edge, relay_edge, to).wait_recv()

            @pl.when(first_stop)
            def _():
                edge_hop(f, relay_edge, relay_edge, to).start()

            @pl.when(second_stop)
            def _():
                edge_hop(f, relay_edge, edge_in, to).start()

    def interior(i, carry):
        main_chunk(i)

        @pl.when(plain_out)
        def _():
            tail_copy(i).start()

        @pl.when(jnp.logical_and(seam_out, i > FAR))
        def _():
            low_copy(i).start()

        @pl.when(jnp.logical_and(seam_out, i <= 3))
        def _():
            @pl.when(i == 1)
            def _():
                pl.semaphore_wait(ready_next.at[0], 1)

            for j in range(3):
                hop(i, j, tail_out, relay, r + 1).start()

        @pl.when(jnp.logical_and(seam_out, jnp.logical_and(i >= 4, i <= FAR)))
        def _():
            @pl.when(i == 4)
            def _():
                pl.semaphore_wait(ready_next.at[1], 1)

            for j in range(3):
                hop(i, j, tail_out, relay, r + 2).start()

        return carry

    lax.fori_loop(1, 4, interior, 0)

    @pl.when(d < n_depth - 1)
    def _():
        up.wait_recv()

    @pl.when(d > 0)
    def _():
        down.wait_recv()

    fold = span // 2
    high = (lane % 16) >= 8

    def fold_edge(load, target, first):
        def body(f, carry):
            packed = pack_columns(lambda g: load(f, g), lane, 0, 8)
            target[f + first] = jnp.where(high[:fold], packed[:fold], pltpu.roll(packed[fold:], 120, 1))
            return carry

        return body

    @pl.when(r > 0)
    def _():
        lax.fori_loop(0, 5, fold_edge(lambda f, g: ext[f, pl.ds(g * ROWS, span)], edge_out, 0), 0)

    @pl.when(plain_out)
    def _():
        edge_copy.start()

    @pl.when(seam_out)
    def _():
        pl.semaphore_wait(ready_next.at[2], 1)
        for f in range(5):
            edge_hop(f, edge_out, relay_edge, r + 3).start()

    lax.fori_loop(4, chunks - 1, interior, 0)

    @pl.when(jnp.logical_and(first_stop, z == 1))
    def _():
        pl.semaphore_wait(ready_next.at[0], 1)
        pass_chunks()

    def rim(i, carry):
        main_chunk(i * (chunks - 1))

        @pl.when(plain_out)
        def _():
            tail_copy(i * (chunks - 1)).start()

        @pl.when(seam_out)
        def _():
            low_copy(i * (chunks - 1)).start()

        return carry

    lax.fori_loop(0, 2, rim, 0)

    @pl.when(jnp.logical_and(passes, z > 1))
    def _():
        pl.semaphore_wait(ready_next.at[0], 1)

        @pl.when(leg < 3)
        def _():
            pass_chunks()

        @pl.when(leg == 3)
        def _():
            pass_edge()

    @pl.when(at_end)
    def _():
        @pl.when(d < n_depth - 1)
        def _():
            far_up.wait_recv()

        @pl.when(d > 0)
        def _():
            far_down.wait_recv()

        nothing = jnp.zeros((span, 128), jnp.float32)

        def far_chunk(i, carry):
            at = pl.multiple_of(i * ROWS, ROWS)
            fields = [nothing] * 3 + [beyond[f, pl.ds(at, span)] for f in range(2)]
            row = iota_row + (row_start - HALO + at)
            results = advance(fields, row, lane + full, offsets, None, full, False, True)
            for f, value in enumerate(results):
                tail[i, f, pl.ds(0, width)] = pack(rolled(value), width, lane)
            return carry

        lax.fori_loop(0, chunks, far_chunk, 0)
        for f in range(3):
            edge_in[f] = nothing[:fold]
        lax.fori_loop(0, 2, fold_edge(lambda f, g: beyond[f, pl.ds(g * ROWS, span)], edge_in, 3), 0)

        @pl.when(d > 0)
        def _():
            far_up.wait_send()

        @pl.when(d < n_depth - 1)
        def _():
            far_down.wait_send()

    near = [i for i in range(chunks) if not 1 <= i <= FAR]

    @pl.when(base)
    def _():
        pl.semaphore_wait(ready_wrap, 1)
        for i in near[1:-1] + [near[0], near[-1]]:
            low_copy(i).wait_recv()
            wrap_copy(i).start()

    @pl.when(plain_in)
    def _():
        edge_copy.wait_recv()

    @pl.when(seam_in)
    def _():
        for f in range(5):
            edge_hop(f, relay_edge, edge_in, r).wait_recv()

    def own_edge(f, carry):
        packed = pack_columns(lambda g: ext[f, pl.ds(g * ROWS, span)], lane, 120, 0)
        folded = edge_in[f]
        other = jnp.concatenate([folded, pltpu.roll(folded, 8, 1)], 0)
        seam[f] = jnp.where(high, other, packed)
        return carry

    lax.fori_loop(0, 5, own_edge, 0)
    row = iota_row + (row_start - HALO) + ROWS * (lane // 16)
    seam_col = 128 * r + 120 + lane % 16

    def seam_inject(t):
        total = jnp.zeros((span, 128), jnp.float32)
        for where_row, where_col, amounts in points:
            here = jnp.logical_and(row == where_row, seam_col == where_col)
            total = total + jnp.where(here, amounts[t], 0.0)
        return total

    results = advance(
        [seam[f] for f in range(5)], row, seam_col, offsets, seam_inject, full, False, True
    )
    for f, value in enumerate(results):
        strip[f] = value[HALO : HALO + ROWS]
    first_lane = 124 - whole
    seen = jnp.logical_and(lane[:ROWS] >= first_lane, lane[:ROWS] < first_lane + 8)

    def place(i, carry):
        at = pl.ds(pl.multiple_of(i * ROWS, ROWS), ROWS)
        amount = lax.rem(248 - whole - 16 * i + 128, 128)
        for f in range(3):
            main[f, at] = jnp.where(seen, pltpu.roll(strip[f], amount, 1), main[f, at])
        return carry

    lax.fori_loop(0, chunks, place, 0)

    @pl.when(plain_in)
    def _():
        for i in range(chunks):
            tail_copy(i).wait_recv()

    @pl.when(seam_in)
    def _():
        for i in near:
            tail_copy(i).wait_recv()
        for i in range(1, FAR + 1):
            for j in range(3):
                hop(i, j, relay, tail, r).wait_recv()

    @pl.when(plain_out)
    def _():
        edge_copy.wait_send()
        for i in range(chunks):
            tail_copy(i).wait_send()

    @pl.when(seam_out)
    def _():
        for i in near:
            low_copy(i).wait_send()
        for i in range(1, FAR + 1):
            for j in range(3):
                hop(i, j, tail_out, relay, r).wait_send()
        for f in range(5):
            edge_hop(f, edge_out, relay_edge, r).wait_send()

    @pl.when(base)
    def _():
        for i in near:
            wrap_copy(i).wait_send()

    @pl.when(passes)
    def _():
        def passed(i, carry):
            for j in range(3):
                hop(i, j, relay, relay, r).wait_send()
            return carry

        lax.fori_loop(first_chunk, last_chunk, passed, 0)

        @pl.when(leg == 3)
        def _():
            for f in range(5):
                edge_hop(f, relay_edge, relay_edge, r).wait_send()

    @pl.when(d > 0)
    def _():
        up.wait_send()

    @pl.when(d < n_depth - 1)
    def _():
        down.wait_send()


def finish(main, tail, shifts, p_out, vr_out, vz_out, out, sem):
    chunks = tail.shape[0]
    whole = shifts[0]
    for t in range(1, ITERS):
        whole = whole + shifts[t]
    lane = lax.broadcasted_iota(jnp.int32, (ROWS, 128), 1)
    far = lane >= 132 - whole
    outs = (p_out, vr_out, vz_out)

    def store(i, f):
        at = pl.ds(pl.multiple_of(i * ROWS, ROWS), ROWS)
        return pltpu.make_async_copy(out.at[f, at], outs[f].at[at], sem.at[i, f])

    for n, width in enumerate(WIDTHS):
        fits = whole <= width + 4
        if n > 0:
            fits = jnp.logical_and(fits, whole > WIDTHS[n - 1] + 4)

        @pl.when(fits)
        def _(width=width):
            def body(i, carry):
                at = pl.ds(pl.multiple_of(i * ROWS, ROWS), ROWS)
                for f in range(3):
                    spread = unpack(tail[i, f, pl.ds(0, width)], width, lane)
                    out[f, at] = jnp.where(far, spread, main[f, at])
                    store(i, f).start()
                return carry

            lax.fori_loop(0, chunks, body, 0)

    for i in range(chunks):
        for f in range(3):
            store(i, f).wait()


def solution(mesh):
    n_range, n_depth = mesh.shape["range"], mesh.shape["depth"]

    def first(ident, width, *args):
        height = args[0].shape[0]
        chunks = height // ROWS
        span = ROWS + 2 * HALO
        f32 = jnp.float32
        dma = pltpu.SemaphoreType.DMA
        hbm = pl.BlockSpec(memory_space=pltpu.HBM)
        vmem = pl.BlockSpec(memory_space=pltpu.VMEM)
        smem = pl.BlockSpec(memory_space=pltpu.SMEM)
        edge = pltpu.VMEM((5, span // 2, 128), f32)
        block = pltpu.VMEM((chunks, 3, WIDTHS[-1], 128), f32)
        return pl.pallas_call(
            functools.partial(kernel, width, n_range, n_depth),
            out_shape=(
                jax.ShapeDtypeStruct((3, height, 128), f32),
                jax.ShapeDtypeStruct((chunks, 3, WIDTHS[-1], 128), f32),
            ),
            in_specs=[hbm] * 7 + [smem] * 3,
            out_specs=(vmem, vmem),
            scratch_shapes=[
                pltpu.VMEM((5, height + 2 * HALO, 128), f32),
                pltpu.VMEM((2, height + 2 * HALO, 128), f32),
                pltpu.VMEM((2, AHEAD, height), f32),
                block, edge, edge, block, edge,
                pltpu.VMEM((5, span, 128), f32),
                pltpu.VMEM((3, ROWS, 128), f32),
                pltpu.VMEM((ITERS, 128, 128), jnp.bfloat16),
                dma((5,)), dma((2,)), dma((2,)), dma((2,)), dma((2,)), dma((2,)),
                dma, dma, dma((chunks,)), dma((chunks,)), dma((chunks, 3)), dma((chunks, 3)), dma((5,)), dma((5,)),
                pltpu.SemaphoreType.REGULAR, pltpu.SemaphoreType.REGULAR((3,)),
            ],
            compiler_params=pltpu.CompilerParams(
                collective_id=ident, has_side_effects=True, vmem_limit_bytes=56 * 2**20
            ),
        )(*args)

    def step(p, vr, vz, c, rho, ac, ad, shifts, sources, wavelet):
        height = p.shape[0]
        total = jnp.sum(shifts)
        which = jnp.int32(0)
        for width in WIDTHS[:-1]:
            which = which + (total > width + 4).astype(jnp.int32)
        main, tail = lax.switch(
            which,
            [functools.partial(first, n + 1, width) for n, width in enumerate(WIDTHS)],
            p, vr, vz, c, rho, ac.T, ad.T, shifts, sources.T, wavelet.T,
        )
        vmem = pl.BlockSpec(memory_space=pltpu.VMEM)
        hbm = pl.BlockSpec(memory_space=pltpu.HBM)
        block = jax.ShapeDtypeStruct((height, 128), jnp.float32)
        return pl.pallas_call(
            finish,
            out_shape=(block, block, block),
            in_specs=[vmem, vmem, pl.BlockSpec(memory_space=pltpu.SMEM)],
            out_specs=(hbm, hbm, hbm),
            scratch_shapes=[
                pltpu.VMEM((3, height, 128), jnp.float32),
                pltpu.SemaphoreType.DMA((height // ROWS, 3)),
            ],
            compiler_params=pltpu.CompilerParams(vmem_limit_bytes=16 * 2**20),
        )(main, tail, shifts)

    block = P("depth", "range")
    return jax.shard_map(
        step,
        mesh=mesh,
        in_specs=(block,) * 5 + (P("depth", None),) * 2 + (P(),) * 3,
        out_specs=(block, block, block),
        check_vma=False,
    )
```

```python
import functools

import jax
import jax.numpy as jnp
from jax import lax
from jax.experimental import pallas as pl
from jax.experimental.pallas import tpu as pltpu
from jax.sharding import PartitionSpec as P

ITERS = 4
TIME_STEP = 0.6
MESH = pl.DeviceIdType.MESH
HALO = 8
ROWS = 128
WIDTHS = (40, 48, 64)
AHEAD = 64
RING = 8


def advance(fields, row, col, offsets, inject, full, left, ends):
    p, vr, vz, c, rho = fields
    n = p.shape[0]
    a = (2.0 * TIME_STEP) / (rho + pltpu.roll(rho, 127, 1))
    b = (2.0 * TIME_STEP) / (rho + pltpu.roll(rho, n - 1, 0))
    b = jnp.where(row >= 0, b, 0.0)
    k = TIME_STEP * (rho * c * c)
    if ends:
        a_last = TIME_STEP / rho
    for t in range(ITERS):
        push_r = pltpu.roll(p, 127, 1) - p
        push_z = b * (pltpu.roll(p, n - 1, 0) - p)
        if ends:
            on = col < full + offsets[t]
            push_r = jnp.where(col == full + offsets[t] - 1, a_last, a) * push_r
            vr = jnp.where(on, vr - push_r, vr)
            vz = jnp.where(on, vz - push_z, vz)
        else:
            vr = vr - a * push_r
            vz = vz - push_z
        back = pltpu.roll(vr, 1, 1)
        if left:
            back = jnp.where(col == offsets[t], 0.0, back)
        fresh = p - k * ((vr - back) + (vz - pltpu.roll(vz, 1, 0)))
        if ends:
            fresh = jnp.where(on, fresh, p)
        p = fresh
        if inject is not None:
            p = p + inject(t)
    return p, vr, vz


def pack_columns(load, lane, start, place):
    total = None
    for g in range(8):
        moved = pltpu.roll(load(g), (16 * g + place - start) % 128, 1)
        total = moved if total is None else jnp.where(lane >= 16 * g + place, moved, total)
    return total


def pieces(width):
    found, end, first = [], 128, 0
    for lanes in (64, 32, 16, 8):
        if width - first >= lanes:
            found.append((lanes, end, first))
            end, first = end - lanes, first + lanes
    return found


def pack(value, width, lane):
    parts = []
    for lanes, end, _ in pieces(width):
        total = None
        for q in range(ROWS // lanes):
            moved = pltpu.roll(value[lanes * q : lanes * (q + 1)], (128 - end - lanes * q) % 128, 1)
            total = moved if q == 0 else jnp.where(lane[:lanes] < 128 - lanes * q, moved, total)
        parts.append(total)
    return parts[0] if len(parts) == 1 else jnp.concatenate(parts, 0)


def unpack(value, width, lane):
    result = None
    for lanes, end, first in reversed(pieces(width)):
        block = value[first : first + lanes]
        rows = [
            pltpu.roll(block, (lanes * q + end) % 128, 1) for q in range(ROWS // lanes)
        ]
        spread = jnp.concatenate(rows, 0)
        result = spread if result is None else jnp.where(lane >= end - lanes, spread, result)
    return result


def kernel(
    width, n_range, n_depth,
    p_in, vr_in, vz_in, c_in, rho_in, ac_in, ad_in, shifts, sources, wavelet,
    main, tail, size,
    ext, beyond, raw, tail_out, edge_out, edge_in, relay, relay_edge, turned, seam, strip, spread,
    in_sem, raw_sem, halo_send, halo_recv, far_send, far_recv, edge_send, edge_recv, tail_send, tail_recv,
    pass_send, pass_recv, edge_pass_send, edge_pass_recv, ready_wrap, ready_next,
):
    r = lax.axis_index("range")
    d = lax.axis_index("depth")
    z = lax.rem(r, RING)
    height = p_in.shape[0]
    chunks = height // ROWS
    at_end = r == n_range - 1
    full = 128 * n_range
    span = ROWS + 2 * HALO
    half = ROWS // 2

    seam_out = jnp.logical_and(z == 0, r > 0)
    seam_in = jnp.logical_and(z == RING - 1, r < n_range - 1)
    upper = r >= RING
    lower = r < n_range - RING
    base = jnp.logical_and(z == 0, lower)
    low_stop = jnp.logical_or(z == 1, z == 2)
    first_stop = jnp.logical_and(low_stop, upper)
    second_stop = jnp.logical_and(low_stop, lower)
    third_stop = jnp.logical_and(jnp.logical_or(z == 4, z == 5), lower)
    foot = z == 0
    top = z == RING - 1
    top_out = jnp.logical_and(top, upper)
    plain_out = z > 0
    plain_in = z < RING - 1

    def one(flag):
        return jnp.where(flag, 1, 0)

    barrier = pltpu.get_barrier_semaphore()

    def greet(flag, semaphore, **where):
        @pl.when(flag)
        def _():
            pl.semaphore_signal(semaphore, inc=1, device_id=where, device_id_type=MESH)

    greet(plain_in, barrier, range=r + 1)
    greet(base, barrier, range=r + RING)
    greet(foot, barrier, range=r + RING - 1)
    greet(seam_in, barrier, range=r + RING)
    greet(second_stop, barrier, range=r + RING)
    greet(second_stop, barrier, range=r + 3)
    greet(third_stop, barrier, range=r + RING - 1 - z)
    greet(seam_out, barrier, range=r + 2)
    greet(d > 0, barrier, depth=d - 1)
    greet(d < n_depth - 1, barrier, depth=d + 1)

    loads = [
        pltpu.make_async_copy(ref, ext.at[i, pl.ds(HALO, height)], in_sem.at[i])
        for i, ref in enumerate((p_in, vr_in, vz_in, c_in, rho_in))
    ]
    for copy in loads:
        copy.start()
    far_loads = [
        pltpu.make_async_copy(ref, raw.at[i], raw_sem.at[i]) for i, ref in enumerate((ac_in, ad_in))
    ]

    @pl.when(at_end)
    def _():
        for copy in far_loads:
            copy.start()

    pl.semaphore_wait(
        barrier,
        one(plain_out) + one(seam_out) + 2 * one(seam_in) + one(third_stop)
        + one(jnp.logical_and(first_stop, z == 2))
        + one(first_stop) + one(top) + one(top_out)
        + one(d > 0) + one(d < n_depth - 1),
    )

    greet(top, ready_wrap, range=r - RING + 1)
    greet(jnp.logical_and(first_stop, z == 1), ready_next.at[0], range=r - 1)
    greet(jnp.logical_and(first_stop, z == 2), ready_next.at[1], range=r - 2)
    greet(seam_in, ready_next.at[0], range=r - 3)
    greet(seam_in, ready_next.at[0], range=r - 2)
    greet(third_stop, ready_next.at[0], range=r - 3)

    offsets = [jnp.int32(0)]
    for t in range(ITERS):
        offsets.append(offsets[-1] + shifts[t])
    whole = offsets[-1]
    size[...] = jnp.broadcast_to(whole, (8, 128))
    points = [
        (sources[0, i], sources[1, i], [wavelet[t, i] for t in range(ITERS)])
        for i in range(sources.shape[1])
    ]
    row_start = d * height
    iota_row = lax.broadcasted_iota(jnp.int32, (span, 128), 0)
    lane = lax.broadcasted_iota(jnp.int32, (span, 128), 1)
    col = lane + 128 * r

    narrow = jnp.bfloat16
    small_lane, small_row = lane[:8], iota_row[:8]
    source_row = jnp.full((8, 128), -HALO - 1, jnp.int32)
    for i, (where_row, _, _) in enumerate(points):
        source_row = jnp.where(
            jnp.logical_and(small_lane % 8 == i, small_lane < 24), where_row, source_row
        )
    source_row = jnp.broadcast_to(source_row[:1], (span, 128))
    for t in range(ITERS):
        amount = jnp.zeros((8, 128), jnp.float32)
        for i, (_, where_col, amounts) in enumerate(points):
            here = jnp.logical_and(small_row == i, small_lane + 128 * r == where_col)
            amount = jnp.where(here, amounts[t], amount)
        first = amount.astype(narrow).astype(jnp.float32)
        second = (amount - first).astype(narrow).astype(jnp.float32)
        third = amount - first - second
        spread[t] = jnp.concatenate(
            [first, second, third, jnp.zeros((104, 128), jnp.float32)], 0
        ).astype(narrow)

    def injector(row):
        picks = jnp.where(row == source_row, 1.0, 0.0).astype(narrow)
        return lambda t: jnp.dot(picks, spread[t], preferred_element_type=jnp.float32)

    for copy in loads:
        copy.wait()

    def rolled(value):
        return pltpu.roll(value[HALO : HALO + ROWS], 128 - whole, 1)

    def main_chunk(i):
        at = pl.multiple_of(i * ROWS, ROWS)
        fields = [ext[f, pl.ds(at, span)] for f in range(5)]
        row = iota_row + (row_start - HALO + at)
        results = advance(fields, row, col, offsets, injector(row), full, True, False)
        for f, value in enumerate(results):
            value = rolled(value)
            main[f, pl.ds(at, ROWS)] = value
            tail_out[i, f, pl.ds(0, width)] = pack(value, width, lane)

    def remote(src, dst, send, recv, **where):
        return pltpu.make_async_remote_copy(
            src_ref=src, dst_ref=dst, send_sem=send, recv_sem=recv,
            device_id=where, device_id_type=MESH,
        )

    def body(ref, i):
        return ref.at[i, :, pl.ds(0, width)]

    def tail_copy(i):
        return remote(body(tail_out, i), body(tail, i), tail_send.at[i], tail_recv.at[i], range=r - 1)

    def low_copy(i):
        return remote(body(tail_out, i), body(relay, i), tail_send.at[i], pass_recv.at[0, i, 0], range=r - RING)

    def wrap_copy(i):
        return remote(body(relay, i), body(tail, i), pass_send.at[0, i, 0], tail_recv.at[i], range=r + RING - 1)

    def part(ref, i, j):
        return ref.at[i, j, pl.ds(0, width)]

    def hop(i, j, source, target, to, sent=0, lands=0):
        return remote(
            part(source, i, j), part(target, i, j), pass_send.at[sent, i, j], pass_recv.at[lands, i, j], range=to
        )

    def edge_hop(f, source, target, to, sent=0, lands=0):
        return remote(
            source.at[f], target.at[f], edge_pass_send.at[sent, f], edge_pass_recv.at[lands, f], range=to
        )

    edge_copy = remote(edge_out, edge_in, edge_send, edge_recv, range=r - 1)

    up = remote(
        ext.at[:, pl.ds(HALO, HALO)], ext.at[:, pl.ds(HALO + height, HALO)],
        halo_send.at[0], halo_recv.at[0], depth=d - 1,
    )
    down = remote(
        ext.at[:, pl.ds(height, HALO)], ext.at[:, pl.ds(0, HALO)],
        halo_send.at[1], halo_recv.at[1], depth=d + 1,
    )

    @pl.when(d > 0)
    def _():
        up.start()

    @pl.when(d < n_depth - 1)
    def _():
        down.start()

    zeros = jnp.zeros((HALO, 128), jnp.float32)

    @pl.when(d == 0)
    def _():
        for f in range(4):
            ext[f, pl.ds(0, HALO)] = zeros
        ext[4, pl.ds(0, HALO)] = zeros + 1.0

    @pl.when(d == n_depth - 1)
    def _():
        for f in range(4):
            ext[f, pl.ds(HALO + height, HALO)] = zeros
        last = ext[4, pl.ds(height, HALO)]
        ext[4, pl.ds(HALO + height, HALO)] = jnp.broadcast_to(last[HALO - 1 :], (HALO, 128))

    far_up = remote(
        beyond.at[:, pl.ds(HALO, HALO)], beyond.at[:, pl.ds(HALO + height, HALO)],
        far_send.at[0], far_recv.at[0], depth=d - 1,
    )
    far_down = remote(
        beyond.at[:, pl.ds(height, HALO)], beyond.at[:, pl.ds(0, HALO)],
        far_send.at[1], far_recv.at[1], depth=d + 1,
    )


    @pl.when(at_end)
    def _():
        for copy in far_loads:
            copy.wait()

        def turn_block(i, carry):
            at = pl.multiple_of(i * ROWS, ROWS)
            for f, fill in enumerate((0.0, 1.0)):
                block = raw[f, :, pl.ds(at, ROWS)]
                block = jnp.concatenate([block, jnp.full((128 - AHEAD, ROWS), fill, jnp.float32)], 0)
                beyond[f, pl.ds(HALO + at, ROWS)] = block.T
            return carry

        lax.fori_loop(0, chunks, turn_block, 0)
        @pl.when(d > 0)
        def _():
            far_up.start()

        @pl.when(d < n_depth - 1)
        def _():
            far_down.start()

        @pl.when(d == 0)
        def _():
            beyond[0, pl.ds(0, HALO)] = zeros
            beyond[1, pl.ds(0, HALO)] = zeros + 1.0

        @pl.when(d == n_depth - 1)
        def _():
            beyond[0, pl.ds(HALO + height, HALO)] = zeros
            last = beyond[1, pl.ds(height, HALO)]
            beyond[1, pl.ds(HALO + height, HALO)] = jnp.broadcast_to(last[HALO - 1 :], (HALO, 128))

    near = (4, 5, 6, 7)
    ring = (0, 1, 2, 3)
    odd_leg = jnp.logical_or(z == 1, z == 4)
    count = jnp.where(odd_leg, 3, 1)

    def chunk_of(n):
        return jnp.where(odd_leg, n + 1, 0)

    def pass_on(source, target, to, sent, lands):
        def step(n, carry):
            i = chunk_of(n)
            for j in range(3):
                hop(i, j, source, source, to, sent, sent).wait_recv()
                hop(i, j, source, target, to, sent, lands).start()
            return carry

        lax.fori_loop(0, count, step, 0)

    def interior(i, carry):
        main_chunk(i)

        @pl.when(plain_out)
        def _():
            tail_copy(i).start()

        @pl.when(jnp.logical_and(seam_out, i > 3))
        def _():
            low_copy(i).start()

        @pl.when(jnp.logical_and(seam_out, i <= 3))
        def _():
            @pl.when(i == 1)
            def _():
                pl.semaphore_wait(ready_next.at[0], 1)

            for j in range(3):
                hop(i, j, tail_out, relay, r + 1).start()

        return carry

    lax.fori_loop(1, 4, interior, 0)

    @pl.when(d < n_depth - 1)
    def _():
        up.wait_recv()

    @pl.when(d > 0)
    def _():
        down.wait_recv()

    fold = span // 2
    high = (lane % 16) >= 8

    def fold_edge(load, target, first):
        def body(f, carry):
            packed = pack_columns(lambda g: load(f, g), lane, 0, 8)
            target[f + first] = jnp.where(high[:fold], packed[:fold], pltpu.roll(packed[fold:], 120, 1))
            return carry

        return body

    @pl.when(r > 0)
    def _():
        lax.fori_loop(0, 5, fold_edge(lambda f, g: ext[f, pl.ds(g * ROWS, span)], edge_out, 0), 0)

    @pl.when(plain_out)
    def _():
        edge_copy.start()

    lax.fori_loop(4, chunks - 1, interior, 0)

    @pl.when(jnp.logical_and(first_stop, z == 1))
    def _():
        pass_on(relay, turned, r - RING, 0, 1)

    def rim(i, carry):
        main_chunk(i * (chunks - 1))

        @pl.when(plain_out)
        def _():
            tail_copy(i * (chunks - 1)).start()

        @pl.when(seam_out)
        def _():
            @pl.when(i == 0)
            def _():
                pl.semaphore_wait(ready_next.at[1], 1)

                for j in range(3):
                    hop(0, j, tail_out, relay, r + 2).start()

            @pl.when(i == 1)
            def _():
                low_copy(chunks - 1).start()

        return carry

    lax.fori_loop(0, 2, rim, 0)

    @pl.when(foot)
    def _():
        pl.semaphore_wait(ready_wrap, 1)

    @pl.when(seam_out)
    def _():
        for f in range(5):
            edge_hop(f, edge_out, relay_edge, r + RING - 1).start()
    @pl.when(top_out)
    def _():
        for f in range(5):
            edge_hop(f, relay_edge, relay_edge, r, 1, 0).wait_recv()
            edge_hop(f, relay_edge, edge_in, r - RING, 1, 1).start()

    @pl.when(jnp.logical_and(first_stop, z == 2))
    def _():
        pass_on(relay, turned, r - RING, 0, 1)

    @pl.when(second_stop)
    def _():
        pl.semaphore_wait(ready_next.at[0], 1)
        pass_on(turned, relay, r + 3, 1, 0)

    @pl.when(at_end)
    def _():
        @pl.when(d < n_depth - 1)
        def _():
            far_up.wait_recv()

        @pl.when(d > 0)
        def _():
            far_down.wait_recv()

        nothing = jnp.zeros((span, 128), jnp.float32)

        def far_chunk(i, carry):
            at = pl.multiple_of(i * ROWS, ROWS)
            fields = [nothing] * 3 + [beyond[f, pl.ds(at, span)] for f in range(2)]
            row = iota_row + (row_start - HALO + at)
            results = advance(fields, row, lane + full, offsets, None, full, False, True)
            for f, value in enumerate(results):
                tail[i, f, pl.ds(0, width)] = pack(rolled(value), width, lane)
            return carry

        lax.fori_loop(0, chunks, far_chunk, 0)
        for f in range(3):
            edge_in[f] = nothing[:fold]
        lax.fori_loop(0, 2, fold_edge(lambda f, g: beyond[f, pl.ds(g * ROWS, span)], edge_in, 3), 0)

        @pl.when(d > 0)
        def _():
            far_up.wait_send()

        @pl.when(d < n_depth - 1)
        def _():
            far_down.wait_send()


    def own_edge(f, carry):
        seam[f] = pack_columns(lambda g: ext[f, pl.ds(g * ROWS, span)], lane, 120, 0)
        return carry

    lax.fori_loop(0, 5, own_edge, 0)

    @pl.when(plain_in)
    def _():
        edge_copy.wait_recv()

    @pl.when(seam_in)
    def _():
        for f in range(5):
            edge_hop(f, relay_edge, edge_in, r, 1, 1).wait_recv()

    def join_edge(f, carry):
        folded = edge_in[f]
        other = jnp.concatenate([folded, pltpu.roll(folded, 8, 1)], 0)
        seam[f] = jnp.where(high, other, seam[f])
        return carry

    lax.fori_loop(0, 5, join_edge, 0)
    row = iota_row + (row_start - HALO) + ROWS * (lane // 16)
    seam_col = 128 * r + 120 + lane % 16

    def seam_inject(t):
        total = jnp.zeros((span, 128), jnp.float32)
        for where_row, where_col, amounts in points:
            here = jnp.logical_and(row == where_row, seam_col == where_col)
            total = total + jnp.where(here, amounts[t], 0.0)
        return total

    results = advance(
        [seam[f] for f in range(5)], row, seam_col, offsets, seam_inject, full, False, True
    )
    for f, value in enumerate(results):
        strip[f] = value[HALO : HALO + ROWS]
    first_lane = 124 - whole
    seen = jnp.logical_and(lane[:ROWS] >= first_lane, lane[:ROWS] < first_lane + 8)

    def place(i, carry):
        for n in (2 * i, 2 * i + 1):
            at = pl.ds(pl.multiple_of(n * ROWS, ROWS), ROWS)
            amount = lax.rem(248 - whole - 16 * n + 128, 128)
            for f in range(3):
                main[f, at] = jnp.where(seen, pltpu.roll(strip[f], amount, 1), main[f, at])
        return carry

    lax.fori_loop(0, chunks // 2, place, 0)

    @pl.when(base)
    def _():
        for i in near:
            low_copy(i).wait_recv()
            wrap_copy(i).start()

    @pl.when(third_stop)
    def _():
        pl.semaphore_wait(ready_next.at[0], 1)
        pass_on(relay, tail, r + RING - 1 - z, 0, 0)

    @pl.when(plain_in)
    def _():
        for i in range(chunks):
            tail_copy(i).wait_recv()

    @pl.when(seam_in)
    def _():
        for i in near:
            tail_copy(i).wait_recv()
        for i in ring:
            for j in range(3):
                hop(i, j, relay, tail, r).wait_recv()

    @pl.when(plain_out)
    def _():
        edge_copy.wait_send()
        for i in range(chunks):
            tail_copy(i).wait_send()

    @pl.when(seam_out)
    def _():
        for i in near:
            low_copy(i).wait_send()
        for i in ring:
            for j in range(3):
                hop(i, j, tail_out, relay, r).wait_send()
        for f in range(5):
            edge_hop(f, edge_out, relay_edge, r).wait_send()

    @pl.when(base)
    def _():
        for i in near:
            wrap_copy(i).wait_send()

    def passed(side):
        def step(n, carry):
            for j in range(3):
                hop(chunk_of(n), j, relay, relay, r, side, side).wait_send()
            return carry

        lax.fori_loop(0, count, step, 0)

    @pl.when(jnp.logical_or(first_stop, third_stop))
    def _():
        passed(0)

    @pl.when(second_stop)
    def _():
        passed(1)

    @pl.when(top_out)
    def _():
        for f in range(5):
            edge_hop(f, relay_edge, edge_in, r, 1, 1).wait_send()
    @pl.when(d > 0)
    def _():
        up.wait_send()

    @pl.when(d < n_depth - 1)
    def _():
        down.wait_send()


def finish(main, tail, size, p_out, vr_out, vz_out, out, sem):
    chunks = tail.shape[0]
    whole = jnp.max(size[...])
    lane = lax.broadcasted_iota(jnp.int32, (ROWS, 128), 1)
    far = lane >= 132 - whole
    outs = (p_out, vr_out, vz_out)

    def store(i, f):
        at = pl.ds(pl.multiple_of(i * ROWS, ROWS), ROWS)
        return pltpu.make_async_copy(out.at[f, at], outs[f].at[at], sem.at[i, f])

    for n, width in enumerate(WIDTHS):
        fits = whole <= width + 4
        if n > 0:
            fits = jnp.logical_and(fits, whole > WIDTHS[n - 1] + 4)

        @pl.when(fits)
        def _(width=width):
            def body(i, carry):
                at = pl.ds(pl.multiple_of(i * ROWS, ROWS), ROWS)
                for f in range(3):
                    spread = unpack(tail[i, f, pl.ds(0, width)], width, lane)
                    out[f, at] = jnp.where(far, spread, main[f, at])
                    store(i, f).start()
                return carry

            lax.fori_loop(0, chunks, body, 0)

    for i in range(chunks):
        for f in range(3):
            store(i, f).wait()


def solution(mesh):
    n_range, n_depth = mesh.shape["range"], mesh.shape["depth"]

    def first(ident, width, *args):
        height = args[0].shape[0]
        chunks = height // ROWS
        span = ROWS + 2 * HALO
        f32 = jnp.float32
        dma = pltpu.SemaphoreType.DMA
        hbm = pl.BlockSpec(memory_space=pltpu.HBM)
        vmem = pl.BlockSpec(memory_space=pltpu.VMEM)
        smem = pl.BlockSpec(memory_space=pltpu.SMEM)
        edge = pltpu.VMEM((5, span // 2, 128), f32)
        block = pltpu.VMEM((chunks, 3, WIDTHS[-1], 128), f32)
        return pl.pallas_call(
            functools.partial(kernel, width, n_range, n_depth),
            out_shape=(
                jax.ShapeDtypeStruct((3, height, 128), f32),
                jax.ShapeDtypeStruct((chunks, 3, WIDTHS[-1], 128), f32),
                jax.ShapeDtypeStruct((8, 128), jnp.int32),
            ),
            in_specs=[hbm] * 7 + [smem] * 3,
            out_specs=(vmem, vmem, vmem),
            scratch_shapes=[
                pltpu.VMEM((5, height + 2 * HALO, 128), f32),
                pltpu.VMEM((2, height + 2 * HALO, 128), f32),
                pltpu.VMEM((2, AHEAD, height), f32),
                block, edge, edge, block, edge, block,
                pltpu.VMEM((5, span, 128), f32),
                pltpu.VMEM((3, ROWS, 128), f32),
                pltpu.VMEM((ITERS, 128, 128), jnp.bfloat16),
                dma((5,)), dma((2,)), dma((2,)), dma((2,)), dma((2,)), dma((2,)),
                dma, dma, dma((chunks,)), dma((chunks,)), dma((2, chunks, 3)), dma((2, chunks, 3)), dma((2, 5)), dma((2, 5)),
                pltpu.SemaphoreType.REGULAR, pltpu.SemaphoreType.REGULAR((2,)),
            ],
            compiler_params=pltpu.CompilerParams(
                collective_id=ident, has_side_effects=True, vmem_limit_bytes=56 * 2**20
            ),
        )(*args)

    def step(p, vr, vz, c, rho, ac, ad, shifts, sources, wavelet):
        height = p.shape[0]
        total = jnp.sum(shifts)
        which = jnp.int32(0)
        for width in WIDTHS[:-1]:
            which = which + (total > width + 4).astype(jnp.int32)
        main, tail, size = lax.switch(
            which,
            [functools.partial(first, n + 1, width) for n, width in enumerate(WIDTHS)],
            p, vr, vz, c, rho, ac.T, ad.T, shifts, sources.T, wavelet.T,
        )
        vmem = pl.BlockSpec(memory_space=pltpu.VMEM)
        hbm = pl.BlockSpec(memory_space=pltpu.HBM)
        block = jax.ShapeDtypeStruct((height, 128), jnp.float32)
        return pl.pallas_call(
            finish,
            out_shape=(block, block, block),
            in_specs=[vmem, vmem, vmem],
            out_specs=(hbm, hbm, hbm),
            scratch_shapes=[
                pltpu.VMEM((3, height, 128), jnp.float32),
                pltpu.SemaphoreType.DMA((height // ROWS, 3)),
            ],
            compiler_params=pltpu.CompilerParams(vmem_limit_bytes=16 * 2**20),
        )(main, tail, size)

    block = P("depth", "range")
    return jax.shard_map(
        step,
        mesh=mesh,
        in_specs=(block,) * 5 + (P("depth", None),) * 2 + (P(),) * 3,
        out_specs=(block, block, block),
        check_vma=False,
    )
```

```python
import functools

import jax
import jax.numpy as jnp
from jax import lax
from jax.experimental import pallas as pl
from jax.experimental.pallas import tpu as pltpu
from jax.sharding import PartitionSpec as P

ITERS = 4
TIME_STEP = 0.6
MESH = pl.DeviceIdType.MESH
HALO = 8
ROWS = 128
WIDTHS = (32, 40, 48, 64)
AHEAD = 64
RING = 8


def advance(fields, row, col, offsets, inject, full, left, ends):
    p, vr, vz, c, rho = fields
    n = p.shape[0]
    a = (2.0 * TIME_STEP) / (rho + pltpu.roll(rho, 127, 1))
    b = (2.0 * TIME_STEP) / (rho + pltpu.roll(rho, n - 1, 0))
    b = jnp.where(row >= 0, b, 0.0)
    k = TIME_STEP * (rho * c * c)
    if ends:
        a_last = TIME_STEP / rho
    for t in range(ITERS):
        push_r = pltpu.roll(p, 127, 1) - p
        push_z = b * (pltpu.roll(p, n - 1, 0) - p)
        if ends:
            on = col < full + offsets[t]
            push_r = jnp.where(col == full + offsets[t] - 1, a_last, a) * push_r
            vr = jnp.where(on, vr - push_r, vr)
            vz = jnp.where(on, vz - push_z, vz)
        else:
            vr = vr - a * push_r
            vz = vz - push_z
        back = pltpu.roll(vr, 1, 1)
        if left:
            back = jnp.where(col == offsets[t], 0.0, back)
        fresh = p - k * ((vr - back) + (vz - pltpu.roll(vz, 1, 0)))
        if ends:
            fresh = jnp.where(on, fresh, p)
        p = fresh
        if inject is not None:
            p = p + inject(t)
    return p, vr, vz


def pack_columns(load, lane, start, place):
    total = None
    for g in range(8):
        moved = pltpu.roll(load(g), (16 * g + place - start) % 128, 1)
        total = moved if total is None else jnp.where(lane >= 16 * g + place, moved, total)
    return total


def pieces(width):
    found, end, first = [], 128, 0
    for lanes in (64, 32, 16, 8):
        if width - first >= lanes:
            found.append((lanes, end, first))
            end, first = end - lanes, first + lanes
    return found


def pack(value, width, lane):
    parts = []
    for lanes, end, _ in pieces(width):
        total = None
        for q in range(ROWS // lanes):
            moved = pltpu.roll(value[lanes * q : lanes * (q + 1)], (128 - end - lanes * q) % 128, 1)
            total = moved if q == 0 else jnp.where(lane[:lanes] < 128 - lanes * q, moved, total)
        parts.append(total)
    return parts[0] if len(parts) == 1 else jnp.concatenate(parts, 0)


def unpack(value, width, lane):
    result = None
    for lanes, end, first in reversed(pieces(width)):
        block = value[first : first + lanes]
        rows = [
            pltpu.roll(block, (lanes * q + end) % 128, 1) for q in range(ROWS // lanes)
        ]
        spread = jnp.concatenate(rows, 0)
        result = spread if result is None else jnp.where(lane >= end - lanes, spread, result)
    return result


def kernel(
    width, n_range, n_depth,
    p_in, vr_in, vz_in, c_in, rho_in, ac_in, ad_in, shifts, sources, wavelet,
    main, tail, size,
    ext, beyond, raw, tail_out, edge_out, edge_in, relay, relay_edge, turned, seam, strip, spread,
    in_sem, raw_sem, halo_send, halo_recv, far_send, far_recv, edge_send, edge_recv, tail_send, tail_recv,
    pass_send, pass_recv, edge_pass_send, edge_pass_recv, ready_wrap, ready_next,
):
    r = lax.axis_index("range")
    d = lax.axis_index("depth")
    z = lax.rem(r, RING)
    height = p_in.shape[0]
    chunks = height // ROWS
    at_end = r == n_range - 1
    full = 128 * n_range
    span = ROWS + 2 * HALO
    half = ROWS // 2

    seam_out = jnp.logical_and(z == 0, r > 0)
    seam_in = jnp.logical_and(z == RING - 1, r < n_range - 1)
    upper = r >= RING
    lower = r < n_range - RING
    base = jnp.logical_and(z == 0, lower)
    low_stop = jnp.logical_or(z == 1, z == 2)
    first_stop = jnp.logical_and(low_stop, upper)
    second_stop = jnp.logical_and(low_stop, lower)
    third_stop = jnp.logical_and(jnp.logical_or(z == 4, z == 5), lower)
    foot = z == 0
    top = z == RING - 1
    top_out = jnp.logical_and(top, upper)
    plain_out = z > 0
    plain_in = z < RING - 1

    def one(flag):
        return jnp.where(flag, 1, 0)

    barrier = pltpu.get_barrier_semaphore()

    def greet(flag, semaphore, **where):
        @pl.when(flag)
        def _():
            pl.semaphore_signal(semaphore, inc=1, device_id=where, device_id_type=MESH)

    greet(plain_in, barrier, range=r + 1)
    greet(base, barrier, range=r + RING)
    greet(foot, barrier, range=r + RING - 1)
    greet(seam_in, barrier, range=r + RING)
    greet(second_stop, barrier, range=r + RING)
    greet(second_stop, barrier, range=r + 3)
    greet(third_stop, barrier, range=r + RING - 1 - z)
    greet(seam_out, barrier, range=r + 2)
    greet(d > 0, barrier, depth=d - 1)
    greet(d < n_depth - 1, barrier, depth=d + 1)

    loads = [
        pltpu.make_async_copy(ref, ext.at[i, pl.ds(HALO, height)], in_sem.at[i])
        for i, ref in enumerate((p_in, vr_in, vz_in, c_in, rho_in))
    ]
    for copy in loads:
        copy.start()
    far_loads = [
        pltpu.make_async_copy(ref, raw.at[i], raw_sem.at[i]) for i, ref in enumerate((ac_in, ad_in))
    ]

    @pl.when(at_end)
    def _():
        for copy in far_loads:
            copy.start()

    pl.semaphore_wait(
        barrier,
        one(plain_out) + one(seam_out) + 2 * one(seam_in) + one(third_stop)
        + one(jnp.logical_and(first_stop, z == 2))
        + one(first_stop) + one(top) + one(top_out)
        + one(d > 0) + one(d < n_depth - 1),
    )

    greet(top, ready_wrap, range=r - RING + 1)
    greet(jnp.logical_and(first_stop, z == 1), ready_next.at[0], range=r - 1)
    greet(jnp.logical_and(first_stop, z == 2), ready_next.at[1], range=r - 2)
    greet(seam_in, ready_next.at[0], range=r - 3)
    greet(seam_in, ready_next.at[0], range=r - 2)
    greet(third_stop, ready_next.at[0], range=r - 3)

    offsets = [jnp.int32(0)]
    for t in range(ITERS):
        offsets.append(offsets[-1] + shifts[t])
    whole = offsets[-1]
    size[...] = jnp.broadcast_to(whole, (8, 128))
    points = [
        (sources[0, i], sources[1, i], [wavelet[t, i] for t in range(ITERS)])
        for i in range(sources.shape[1])
    ]
    row_start = d * height
    iota_row = lax.broadcasted_iota(jnp.int32, (span, 128), 0)
    lane = lax.broadcasted_iota(jnp.int32, (span, 128), 1)
    col = lane + 128 * r

    narrow = jnp.bfloat16
    small_lane, small_row = lane[:8], iota_row[:8]
    source_row = jnp.full((8, 128), -HALO - 1, jnp.int32)
    for i, (where_row, _, _) in enumerate(points):
        source_row = jnp.where(
            jnp.logical_and(small_lane % 8 == i, small_lane < 24), where_row, source_row
        )
    source_row = jnp.broadcast_to(source_row[:1], (span, 128))
    for t in range(ITERS):
        amount = jnp.zeros((8, 128), jnp.float32)
        for i, (_, where_col, amounts) in enumerate(points):
            here = jnp.logical_and(small_row == i, small_lane + 128 * r == where_col)
            amount = jnp.where(here, amounts[t], amount)
        first = amount.astype(narrow).astype(jnp.float32)
        second = (amount - first).astype(narrow).astype(jnp.float32)
        third = amount - first - second
        spread[t] = jnp.concatenate(
            [first, second, third, jnp.zeros((104, 128), jnp.float32)], 0
        ).astype(narrow)

    def injector(row):
        picks = jnp.where(row == source_row, 1.0, 0.0).astype(narrow)
        return lambda t: jnp.dot(picks, spread[t], preferred_element_type=jnp.float32)

    for copy in loads:
        copy.wait()

    def rolled(value):
        return pltpu.roll(value[HALO : HALO + ROWS], 128 - whole, 1)

    def main_chunk(i):
        at = pl.multiple_of(i * ROWS, ROWS)
        fields = [ext[f, pl.ds(at, span)] for f in range(5)]
        row = iota_row + (row_start - HALO + at)
        results = advance(fields, row, col, offsets, injector(row), full, True, False)
        for f, value in enumerate(results):
            value = rolled(value)
            main[f, pl.ds(at, ROWS)] = value
            tail_out[i, f, pl.ds(0, width)] = pack(value, width, lane)

    def remote(src, dst, send, recv, **where):
        return pltpu.make_async_remote_copy(
            src_ref=src, dst_ref=dst, send_sem=send, recv_sem=recv,
            device_id=where, device_id_type=MESH,
        )

    def body(ref, i):
        return ref.at[i, :, pl.ds(0, width)]

    def tail_copy(i):
        return remote(body(tail_out, i), body(tail, i), tail_send.at[i], tail_recv.at[i], range=r - 1)

    def low_copy(i):
        return remote(body(tail_out, i), body(relay, i), tail_send.at[i], pass_recv.at[0, i, 0], range=r - RING)

    def wrap_copy(i):
        return remote(body(relay, i), body(tail, i), pass_send.at[0, i, 0], tail_recv.at[i], range=r + RING - 1)

    def part(ref, i, j):
        return ref.at[i, j, pl.ds(0, width)]

    def hop(i, j, source, target, to, sent=0, lands=0):
        return remote(
            part(source, i, j), part(target, i, j), pass_send.at[sent, i, j], pass_recv.at[lands, i, j], range=to
        )

    def edge_hop(f, source, target, to, sent=0, lands=0):
        return remote(
            source.at[f], target.at[f], edge_pass_send.at[sent, f], edge_pass_recv.at[lands, f], range=to
        )

    edge_copy = remote(edge_out, edge_in, edge_send, edge_recv, range=r - 1)

    up = remote(
        ext.at[:, pl.ds(HALO, HALO)], ext.at[:, pl.ds(HALO + height, HALO)],
        halo_send.at[0], halo_recv.at[0], depth=d - 1,
    )
    down = remote(
        ext.at[:, pl.ds(height, HALO)], ext.at[:, pl.ds(0, HALO)],
        halo_send.at[1], halo_recv.at[1], depth=d + 1,
    )

    @pl.when(d > 0)
    def _():
        up.start()

    @pl.when(d < n_depth - 1)
    def _():
        down.start()

    zeros = jnp.zeros((HALO, 128), jnp.float32)

    @pl.when(d == 0)
    def _():
        for f in range(4):
            ext[f, pl.ds(0, HALO)] = zeros
        ext[4, pl.ds(0, HALO)] = zeros + 1.0

    @pl.when(d == n_depth - 1)
    def _():
        for f in range(4):
            ext[f, pl.ds(HALO + height, HALO)] = zeros
        last = ext[4, pl.ds(height, HALO)]
        ext[4, pl.ds(HALO + height, HALO)] = jnp.broadcast_to(last[HALO - 1 :], (HALO, 128))

    far_up = remote(
        beyond.at[:, pl.ds(HALO, HALO)], beyond.at[:, pl.ds(HALO + height, HALO)],
        far_send.at[0], far_recv.at[0], depth=d - 1,
    )
    far_down = remote(
        beyond.at[:, pl.ds(height, HALO)], beyond.at[:, pl.ds(0, HALO)],
        far_send.at[1], far_recv.at[1], depth=d + 1,
    )


    @pl.when(at_end)
    def _():
        for copy in far_loads:
            copy.wait()

        def turn_block(i, carry):
            at = pl.multiple_of(i * ROWS, ROWS)
            for f, fill in enumerate((0.0, 1.0)):
                block = raw[f, :, pl.ds(at, ROWS)]
                block = jnp.concatenate([block, jnp.full((128 - AHEAD, ROWS), fill, jnp.float32)], 0)
                beyond[f, pl.ds(HALO + at, ROWS)] = block.T
            return carry

        lax.fori_loop(0, chunks, turn_block, 0)
        @pl.when(d > 0)
        def _():
            far_up.start()

        @pl.when(d < n_depth - 1)
        def _():
            far_down.start()

        @pl.when(d == 0)
        def _():
            beyond[0, pl.ds(0, HALO)] = zeros
            beyond[1, pl.ds(0, HALO)] = zeros + 1.0

        @pl.when(d == n_depth - 1)
        def _():
            beyond[0, pl.ds(HALO + height, HALO)] = zeros
            last = beyond[1, pl.ds(height, HALO)]
            beyond[1, pl.ds(HALO + height, HALO)] = jnp.broadcast_to(last[HALO - 1 :], (HALO, 128))

    near = (4, 5, 6, 7)
    ring = (0, 1, 2, 3)
    odd_leg = jnp.logical_or(z == 1, z == 4)
    count = jnp.where(odd_leg, 3, 1)

    def chunk_of(n):
        return jnp.where(odd_leg, n + 1, 0)

    def pass_on(source, target, to, sent, lands):
        def step(n, carry):
            i = chunk_of(n)
            for j in range(3):
                hop(i, j, source, source, to, sent, sent).wait_recv()
                hop(i, j, source, target, to, sent, lands).start()
            return carry

        lax.fori_loop(0, count, step, 0)

    def interior(i, carry):
        main_chunk(i)

        @pl.when(plain_out)
        def _():
            tail_copy(i).start()

        @pl.when(jnp.logical_and(seam_out, i > 3))
        def _():
            low_copy(i).start()

        @pl.when(jnp.logical_and(seam_out, i <= 3))
        def _():
            @pl.when(i == 1)
            def _():
                pl.semaphore_wait(ready_next.at[0], 1)

            for j in range(3):
                hop(i, j, tail_out, relay, r + 1).start()

        return carry

    lax.fori_loop(1, 4, interior, 0)

    @pl.when(d < n_depth - 1)
    def _():
        up.wait_recv()

    @pl.when(d > 0)
    def _():
        down.wait_recv()

    fold = span // 2
    high = (lane % 16) >= 8

    def fold_edge(load, target, first):
        def body(f, carry):
            packed = pack_columns(lambda g: load(f, g), lane, 0, 8)
            target[f + first] = jnp.where(high[:fold], packed[:fold], pltpu.roll(packed[fold:], 120, 1))
            return carry

        return body

    @pl.when(r > 0)
    def _():
        lax.fori_loop(0, 5, fold_edge(lambda f, g: ext[f, pl.ds(g * ROWS, span)], edge_out, 0), 0)

    @pl.when(plain_out)
    def _():
        edge_copy.start()

    lax.fori_loop(4, chunks - 1, interior, 0)

    @pl.when(jnp.logical_and(first_stop, z == 1))
    def _():
        pass_on(relay, turned, r - RING, 0, 1)

    @pl.when(top_out)
    def _():
        for f in range(5):
            edge_hop(f, relay_edge, relay_edge, r, 1, 0).wait_recv()
            edge_hop(f, relay_edge, edge_in, r - RING, 1, 1).start()

    def rim(i, carry):
        main_chunk(i * (chunks - 1))

        @pl.when(plain_out)
        def _():
            tail_copy(i * (chunks - 1)).start()

        @pl.when(seam_out)
        def _():
            @pl.when(i == 0)
            def _():
                pl.semaphore_wait(ready_next.at[1], 1)

                for j in range(3):
                    hop(0, j, tail_out, relay, r + 2).start()

            @pl.when(i == 1)
            def _():
                low_copy(chunks - 1).start()

        return carry

    lax.fori_loop(0, 2, rim, 0)

    @pl.when(foot)
    def _():
        pl.semaphore_wait(ready_wrap, 1)

    @pl.when(seam_out)
    def _():
        for f in range(5):
            edge_hop(f, edge_out, relay_edge, r + RING - 1).start()
    @pl.when(jnp.logical_and(first_stop, z == 2))
    def _():
        pass_on(relay, turned, r - RING, 0, 1)

    @pl.when(at_end)
    def _():
        @pl.when(d < n_depth - 1)
        def _():
            far_up.wait_recv()

        @pl.when(d > 0)
        def _():
            far_down.wait_recv()

        nothing = jnp.zeros((span, 128), jnp.float32)

        def far_chunk(i, carry):
            at = pl.multiple_of(i * ROWS, ROWS)
            fields = [nothing] * 3 + [beyond[f, pl.ds(at, span)] for f in range(2)]
            row = iota_row + (row_start - HALO + at)
            results = advance(fields, row, lane + full, offsets, None, full, False, True)
            for f, value in enumerate(results):
                tail[i, f, pl.ds(0, width)] = pack(rolled(value), width, lane)
            return carry

        lax.fori_loop(0, chunks, far_chunk, 0)
        for f in range(3):
            edge_in[f] = nothing[:fold]
        lax.fori_loop(0, 2, fold_edge(lambda f, g: beyond[f, pl.ds(g * ROWS, span)], edge_in, 3), 0)

        @pl.when(d > 0)
        def _():
            far_up.wait_send()

        @pl.when(d < n_depth - 1)
        def _():
            far_down.wait_send()


    def own_edge(f, carry):
        seam[f] = pack_columns(lambda g: ext[f, pl.ds(g * ROWS, span)], lane, 120, 0)
        return carry

    lax.fori_loop(0, 5, own_edge, 0)

    @pl.when(plain_in)
    def _():
        edge_copy.wait_recv()

    @pl.when(seam_in)
    def _():
        for f in range(5):
            edge_hop(f, relay_edge, edge_in, r, 1, 1).wait_recv()

    def join_edge(f, carry):
        folded = edge_in[f]
        other = jnp.concatenate([folded, pltpu.roll(folded, 8, 1)], 0)
        seam[f] = jnp.where(high, other, seam[f])
        return carry

    lax.fori_loop(0, 5, join_edge, 0)
    row = iota_row + (row_start - HALO) + ROWS * (lane // 16)
    seam_col = 128 * r + 120 + lane % 16

    def seam_inject(t):
        total = jnp.zeros((span, 128), jnp.float32)
        for where_row, where_col, amounts in points:
            here = jnp.logical_and(row == where_row, seam_col == where_col)
            total = total + jnp.where(here, amounts[t], 0.0)
        return total

    results = advance(
        [seam[f] for f in range(5)], row, seam_col, offsets, seam_inject, full, False, True
    )
    for f, value in enumerate(results):
        strip[f] = value[HALO : HALO + ROWS]
    first_lane = 124 - whole
    seen = jnp.logical_and(lane[:ROWS] >= first_lane, lane[:ROWS] < first_lane + 8)

    def place(i, carry):
        for n in (2 * i, 2 * i + 1):
            at = pl.ds(pl.multiple_of(n * ROWS, ROWS), ROWS)
            amount = lax.rem(248 - whole - 16 * n + 128, 128)
            for f in range(3):
                main[f, at] = jnp.where(seen, pltpu.roll(strip[f], amount, 1), main[f, at])
        return carry

    lax.fori_loop(0, chunks // 2, place, 0)

    @pl.when(second_stop)
    def _():
        pl.semaphore_wait(ready_next.at[0], 1)
        pass_on(turned, relay, r + 3, 1, 0)

    @pl.when(base)
    def _():
        for i in near:
            low_copy(i).wait_recv()
            wrap_copy(i).start()

    @pl.when(third_stop)
    def _():
        pl.semaphore_wait(ready_next.at[0], 1)
        pass_on(relay, tail, r + RING - 1 - z, 0, 0)

    @pl.when(plain_in)
    def _():
        for i in range(chunks):
            tail_copy(i).wait_recv()

    @pl.when(seam_in)
    def _():
        for i in near:
            tail_copy(i).wait_recv()
        for i in ring:
            for j in range(3):
                hop(i, j, relay, tail, r).wait_recv()

    @pl.when(plain_out)
    def _():
        edge_copy.wait_send()
        for i in range(chunks):
            tail_copy(i).wait_send()

    @pl.when(seam_out)
    def _():
        for i in near:
            low_copy(i).wait_send()
        for i in ring:
            for j in range(3):
                hop(i, j, tail_out, relay, r).wait_send()
        for f in range(5):
            edge_hop(f, edge_out, relay_edge, r).wait_send()

    @pl.when(base)
    def _():
        for i in near:
            wrap_copy(i).wait_send()

    def passed(side):
        def step(n, carry):
            for j in range(3):
                hop(chunk_of(n), j, relay, relay, r, side, side).wait_send()
            return carry

        lax.fori_loop(0, count, step, 0)

    @pl.when(jnp.logical_or(first_stop, third_stop))
    def _():
        passed(0)

    @pl.when(second_stop)
    def _():
        passed(1)

    @pl.when(top_out)
    def _():
        for f in range(5):
            edge_hop(f, relay_edge, edge_in, r, 1, 1).wait_send()
    @pl.when(d > 0)
    def _():
        up.wait_send()

    @pl.when(d < n_depth - 1)
    def _():
        down.wait_send()


def finish(main, tail, size, p_out, vr_out, vz_out, out, sem):
    chunks = tail.shape[0]
    whole = jnp.max(size[...])
    lane = lax.broadcasted_iota(jnp.int32, (ROWS, 128), 1)
    far = lane >= 132 - whole
    outs = (p_out, vr_out, vz_out)

    def store(i, f):
        at = pl.ds(pl.multiple_of(i * ROWS, ROWS), ROWS)
        return pltpu.make_async_copy(out.at[f, at], outs[f].at[at], sem.at[i, f])

    for n, width in enumerate(WIDTHS):
        fits = whole <= width + 4
        if n > 0:
            fits = jnp.logical_and(fits, whole > WIDTHS[n - 1] + 4)

        @pl.when(fits)
        def _(width=width):
            def body(i, carry):
                at = pl.ds(pl.multiple_of(i * ROWS, ROWS), ROWS)
                for f in range(3):
                    spread = unpack(tail[i, f, pl.ds(0, width)], width, lane)
                    out[f, at] = jnp.where(far, spread, main[f, at])
                    store(i, f).start()
                return carry

            lax.fori_loop(0, chunks, body, 0)

    for i in range(chunks):
        for f in range(3):
            store(i, f).wait()


def solution(mesh):
    n_range, n_depth = mesh.shape["range"], mesh.shape["depth"]

    def first(ident, width, *args):
        height = args[0].shape[0]
        chunks = height // ROWS
        span = ROWS + 2 * HALO
        f32 = jnp.float32
        dma = pltpu.SemaphoreType.DMA
        hbm = pl.BlockSpec(memory_space=pltpu.HBM)
        vmem = pl.BlockSpec(memory_space=pltpu.VMEM)
        smem = pl.BlockSpec(memory_space=pltpu.SMEM)
        edge = pltpu.VMEM((5, span // 2, 128), f32)
        block = pltpu.VMEM((chunks, 3, WIDTHS[-1], 128), f32)
        return pl.pallas_call(
            functools.partial(kernel, width, n_range, n_depth),
            out_shape=(
                jax.ShapeDtypeStruct((3, height, 128), f32),
                jax.ShapeDtypeStruct((chunks, 3, WIDTHS[-1], 128), f32),
                jax.ShapeDtypeStruct((8, 128), jnp.int32),
            ),
            in_specs=[hbm] * 7 + [smem] * 3,
            out_specs=(vmem, vmem, vmem),
            scratch_shapes=[
                pltpu.VMEM((5, height + 2 * HALO, 128), f32),
                pltpu.VMEM((2, height + 2 * HALO, 128), f32),
                pltpu.VMEM((2, AHEAD, height), f32),
                block, edge, edge, block, edge, block,
                pltpu.VMEM((5, span, 128), f32),
                pltpu.VMEM((3, ROWS, 128), f32),
                pltpu.VMEM((ITERS, 128, 128), jnp.bfloat16),
                dma((5,)), dma((2,)), dma((2,)), dma((2,)), dma((2,)), dma((2,)),
                dma, dma, dma((chunks,)), dma((chunks,)), dma((2, chunks, 3)), dma((2, chunks, 3)), dma((2, 5)), dma((2, 5)),
                pltpu.SemaphoreType.REGULAR, pltpu.SemaphoreType.REGULAR((2,)),
            ],
            compiler_params=pltpu.CompilerParams(
                collective_id=ident, has_side_effects=True, vmem_limit_bytes=56 * 2**20
            ),
        )(*args)

    def step(p, vr, vz, c, rho, ac, ad, shifts, sources, wavelet):
        height = p.shape[0]
        which = (jnp.sum(shifts) - (WIDTHS[0] - 3)) >> 3
        main, tail, size = lax.switch(
            which,
            [functools.partial(first, n + 1, width) for n, width in enumerate(WIDTHS)],
            p, vr, vz, c, rho, ac.T, ad.T, shifts, sources.T, wavelet.T,
        )
        vmem = pl.BlockSpec(memory_space=pltpu.VMEM)
        hbm = pl.BlockSpec(memory_space=pltpu.HBM)
        block = jax.ShapeDtypeStruct((height, 128), jnp.float32)
        return pl.pallas_call(
            finish,
            out_shape=(block, block, block),
            in_specs=[vmem, vmem, vmem],
            out_specs=(hbm, hbm, hbm),
            scratch_shapes=[
                pltpu.VMEM((3, height, 128), jnp.float32),
                pltpu.SemaphoreType.DMA((height // ROWS, 3)),
            ],
            compiler_params=pltpu.CompilerParams(vmem_limit_bytes=16 * 2**20),
        )(main, tail, size)

    block = P("depth", "range")
    return jax.shard_map(
        step,
        mesh=mesh,
        in_specs=(block,) * 5 + (P("depth", None),) * 2 + (P(),) * 3,
        out_specs=(block, block, block),
        check_vma=False,
    )
```
